16 devices in a mesh: data: 16 (over z, y, x, core).
Axes of the slice: x: 2, y: 2, z: 2, core: 2. Of those that a mesh axis runs over, the one named last changes fastest.
Arguments:
- x_in: bfloat16 [32, 384, 1024], P('data')
- grad_y: bfloat16 [32, 384, 1024], P('data')
- gain_one: float32 [2, 1024], replicated
- gain_two: float32 [2, 1024], replicated
- w_qkv: bfloat16 [2, 1024, 3072], replicated
- w_out: bfloat16 [2, 1024, 1024], replicated
- w_up: bfloat16 [2, 1024, 4096], replicated
- w_down: bfloat16 [2, 4096, 1024], replicated
Outputs:
- output 1: bfloat16 [32, 384, 1024], P('data')
- output 2: float32 [2, 1024], replicated
- output 3: float32 [2, 1024], replicated
- output 4: float32 [2, 1024, 3072], replicated
- output 5: float32 [2, 1024, 1024], replicated
- output 6: float32 [2, 1024, 4096], replicated
- output 7: float32 [2, 4096, 1024], replicated
All inputs are finite; a program needn't handle non-finite values.
Results may differ from the reference program's by a relative error of at most 0.02.
Values are sent between devices in bfloat16 or wider.
A program may use at most 1 GiB of HBM per device.

```python
import jax
import jax.numpy as jnp
from jax import lax

D = 1024
FF = 4096
HEADS = 16
LAYERS = 2
SEQ = 384
BATCH = 32
GROUP = 16
HEAD_DIM = D // HEADS
NORM_EPS = 1e-6


def setup_inputs(seed: int = 0) -> dict:
    root_key = jax.random.key(seed)
    sub_keys = jax.random.split(root_key, 8)
    x_in = jax.random.normal(sub_keys[0], (BATCH, SEQ, D), jnp.float32)
    grad_y = jax.random.normal(sub_keys[1], (BATCH, SEQ, D), jnp.float32)
    gain_one = 1.0 + 0.3 * jax.random.normal(sub_keys[2], (LAYERS, D), jnp.float32)
    gain_two = 1.0 + 0.3 * jax.random.normal(sub_keys[3], (LAYERS, D), jnp.float32)
    w_qkv = jax.random.normal(sub_keys[4], (LAYERS, D, 3 * D), jnp.float32) * D ** -0.5
    w_out = jax.random.normal(sub_keys[5], (LAYERS, D, D), jnp.float32) * D ** -0.5
    w_up = jax.random.normal(sub_keys[6], (LAYERS, D, FF), jnp.float32) * D ** -0.5
    w_down = jax.random.normal(sub_keys[7], (LAYERS, FF, D), jnp.float32) * FF ** -0.5
    return {'x_in': x_in.astype(jnp.bfloat16), 'grad_y': grad_y.astype(jnp.bfloat16), 'gain_one': gain_one, 'gain_two': gain_two, 'w_qkv': w_qkv.astype(jnp.bfloat16), 'w_out': w_out.astype(jnp.bfloat16), 'w_up': w_up.astype(jnp.bfloat16), 'w_down': w_down.astype(jnp.bfloat16)}


def rms_gain(rows_f, gain_vec):
    return rows_f * lax.rsqrt(jnp.mean(rows_f * rows_f, axis=-1, keepdims=True) + NORM_EPS) * gain_vec


def gelu_tanh(pre_act):
    return jax.nn.gelu(pre_act, approximate=True)


def mat_lo(lhs_mat, rhs_mat):
    return jnp.dot(lhs_mat, rhs_mat, preferred_element_type=jnp.float32).astype(jnp.bfloat16)


def mat_nt(lhs_mat, rhs_mat):
    return lax.dot_general(lhs_mat, rhs_mat, (((1,), (1,)), ((), ())), preferred_element_type=jnp.float32).astype(jnp.bfloat16)


def mat_tn(lhs_mat, rhs_mat):
    return lax.dot_general(lhs_mat, rhs_mat, (((0,), (0,)), ((), ())), preferred_element_type=jnp.float32)


def head_mix(einsum_spec, lhs_arr, rhs_arr):
    return jnp.einsum(einsum_spec, lhs_arr.astype(jnp.float32), rhs_arr.astype(jnp.float32))


def seq_forward(seq_rows, gain_a, gain_b, w_qkv, w_out, w_up):
    norm_a, norm_a_back = jax.vjp(rms_gain, seq_rows.astype(jnp.float32), gain_a)
    u_one = norm_a.astype(jnp.bfloat16)
    qkv_lo = mat_lo(u_one, w_qkv)
    q_all = qkv_lo[:, :D].reshape(SEQ, HEADS, HEAD_DIM)
    k_all = qkv_lo[:, D:2 * D].reshape(SEQ, HEADS, HEAD_DIM)
    v_all = qkv_lo[:, 2 * D:].reshape(SEQ, HEADS, HEAD_DIM)
    scores = head_mix('qhe,khe->hqk', q_all, k_all) * HEAD_DIM ** -0.5
    causal = jnp.arange(SEQ)[:, None] >= jnp.arange(SEQ)[None, :]
    prob_full = jax.nn.softmax(jnp.where(causal, scores, -1e30), axis=-1)
    prob_lo = prob_full.astype(jnp.bfloat16)
    attn_out = head_mix('hqk,khe->qhe', prob_lo, v_all).astype(jnp.bfloat16).reshape(SEQ, D)
    hidden = seq_rows + mat_lo(attn_out, w_out)
    norm_b, norm_b_back = jax.vjp(rms_gain, hidden.astype(jnp.float32), gain_b)
    u_two = norm_b.astype(jnp.bfloat16)
    pre_lo = mat_lo(u_two, w_up)
    act_f, gelu_back = jax.vjp(gelu_tanh, pre_lo.astype(jnp.float32))
    act_lo = act_f.astype(jnp.bfloat16)
    saved_vals = (norm_a_back, u_one, q_all, k_all, v_all, prob_full, prob_lo, attn_out, norm_b_back, u_two, gelu_back, act_lo)
    return hidden, act_lo, saved_vals


def seq_backward(grad_blk, saved_vals, w_qkv, w_out, w_up, w_down):
    (norm_a_back, u_one, q_all, k_all, v_all, prob_full, prob_lo, attn_out, norm_b_back, u_two, gelu_back, act_lo) = saved_vals
    grad_down_w = mat_tn(act_lo, grad_blk)
    grad_act = mat_nt(grad_blk, w_down)
    (grad_pre_f,) = gelu_back(grad_act.astype(jnp.float32))
    grad_pre = grad_pre_f.astype(jnp.bfloat16)
    grad_up_w = mat_tn(u_two, grad_pre)
    grad_u_two = mat_nt(grad_pre, w_up)
    grad_h_norm, grad_gain_b = norm_b_back(grad_u_two.astype(jnp.float32))
    grad_hidden = (grad_blk.astype(jnp.float32) + grad_h_norm).astype(jnp.bfloat16)
    grad_out_w = mat_tn(attn_out, grad_hidden)
    grad_attn = mat_nt(grad_hidden, w_out).reshape(SEQ, HEADS, HEAD_DIM)
    grad_probs = head_mix('qhe,khe->hqk', grad_attn, v_all)
    grad_scores = (prob_full * (grad_probs - jnp.sum(prob_full * grad_probs, axis=-1, keepdims=True)) * HEAD_DIM ** -0.5).astype(jnp.bfloat16)
    grad_v = head_mix('hqk,qhe->khe', prob_lo, grad_attn).astype(jnp.bfloat16)
    grad_q = head_mix('hqk,khe->qhe', grad_scores, k_all).astype(jnp.bfloat16)
    grad_k = head_mix('hqk,qhe->khe', grad_scores, q_all).astype(jnp.bfloat16)
    grad_qkv = jnp.concatenate([grad_q.reshape(SEQ, D), grad_k.reshape(SEQ, D), grad_v.reshape(SEQ, D)], axis=-1)
    grad_qkv_w = mat_tn(u_one, grad_qkv)
    grad_u_one = mat_nt(grad_qkv, w_qkv)
    grad_x_norm, grad_gain_a = norm_a_back(grad_u_one.astype(jnp.float32))
    grad_x_blk = (grad_hidden.astype(jnp.float32) + grad_x_norm).astype(jnp.bfloat16)
    return grad_x_blk, (grad_gain_a, grad_gain_b, grad_qkv_w, grad_out_w, grad_up_w, grad_down_w)


def reference(x_in, grad_y, gain_one, gain_two, w_qkv, w_out, w_up, w_down):
    def one_seq(grad_acc, seq_pair):
        seq_rows, seq_grad = seq_pair
        hidden_x = seq_rows
        saved_all = []
        for layer_idx in range(LAYERS):
            hidden, act_lo, saved_vals = seq_forward(hidden_x, gain_one[layer_idx], gain_two[layer_idx], w_qkv[layer_idx], w_out[layer_idx], w_up[layer_idx])
            saved_all.append(saved_vals)
            if layer_idx + 1 < LAYERS:
                hidden_x = hidden + mat_lo(act_lo, w_down[layer_idx])
        grad_cur = seq_grad
        grads_rev = []
        for layer_idx in reversed(range(LAYERS)):
            grad_cur, layer_grads = seq_backward(grad_cur, saved_all[layer_idx], w_qkv[layer_idx], w_out[layer_idx], w_up[layer_idx], w_down[layer_idx])
            grads_rev.append(layer_grads)
        grads_fwd = grads_rev[::-1]
        new_acc = tuple(grad_acc[grad_idx] + jnp.stack([layer_set[grad_idx] for layer_set in grads_fwd]) for grad_idx in range(6))
        return new_acc, grad_cur

    init_acc = (jnp.zeros((LAYERS, D), jnp.float32), jnp.zeros((LAYERS, D), jnp.float32), jnp.zeros((LAYERS, D, 3 * D), jnp.float32), jnp.zeros((LAYERS, D, D), jnp.float32), jnp.zeros((LAYERS, D, FF), jnp.float32), jnp.zeros((LAYERS, FF, D), jnp.float32))
    grad_sums, grad_x = lax.scan(one_seq, init_acc, (x_in, grad_y))
    return (grad_x, grad_sums[0] / GROUP, grad_sums[1] / GROUP, grad_sums[2] / GROUP, grad_sums[3] / GROUP, grad_sums[4] / GROUP, grad_sums[5] / GROUP)
```

```python
import functools

import jax
import jax.numpy as jnp
from jax import lax
from jax.experimental import pallas as pl
from jax.experimental.pallas import tpu as pltpu
from jax.sharding import PartitionSpec as P

NORM_EPS = 1e-6
HEAD_DIM = 64
N_DEV = 16


def rms_gain(rows_f, gain_vec):
    return rows_f * lax.rsqrt(jnp.mean(rows_f * rows_f, axis=-1, keepdims=True) + NORM_EPS) * gain_vec


def gelu_tanh(pre_act):
    return jax.nn.gelu(pre_act, approximate=True)


def dot_lo(lhs, rhs):
    return lax.dot_general(lhs, rhs, (((1,), (0,)), ((), ())), preferred_element_type=jnp.float32).astype(jnp.bfloat16)


def dot_nt(lhs, rhs):
    return lax.dot_general(lhs, rhs, (((1,), (1,)), ((), ())), preferred_element_type=jnp.float32).astype(jnp.bfloat16)


def dot_tn(lhs, rhs):
    return lax.dot_general(lhs, rhs, (((0,), (0,)), ((), ())), preferred_element_type=jnp.float32)


Q_BLOCK = 128


def head_mask(which):
    lane = lax.broadcasted_iota(jnp.int32, (Q_BLOCK, 2 * HEAD_DIM), 1)
    return (lane >= which * HEAD_DIM) & (lane < (which + 1) * HEAD_DIM)


def block_probs(q_rows, k_ref, blk, mask):
    n_key = (blk + 1) * Q_BLOCK
    q_one = jnp.where(mask, q_rows, jnp.zeros_like(q_rows))
    scores = lax.dot_general(q_one, k_ref[:n_key, :], (((1,), (1,)), ((), ())), preferred_element_type=jnp.float32) * HEAD_DIM ** -0.5
    row = lax.broadcasted_iota(jnp.int32, (Q_BLOCK, n_key), 0) + blk * Q_BLOCK
    col = lax.broadcasted_iota(jnp.int32, (Q_BLOCK, n_key), 1)
    scores = jnp.where(row >= col, scores, -1e30)
    expo = jnp.exp(scores - jnp.max(scores, axis=-1, keepdims=True))
    return expo * (1.0 / jnp.sum(expo, axis=-1, keepdims=True))


def attn_fwd_kernel(q_ref, k_ref, v_ref, o_ref):
    mask = head_mask(0)
    for blk in range(q_ref.shape[0] // Q_BLOCK):
        rows = pl.ds(blk * Q_BLOCK, Q_BLOCK)
        n_key = (blk + 1) * Q_BLOCK
        both = []
        for which in range(2):
            prob = block_probs(q_ref[rows, :], k_ref, blk, head_mask(which)).astype(jnp.bfloat16)
            both.append(jnp.dot(prob, v_ref[:n_key, :], preferred_element_type=jnp.float32))
        o_ref[rows, :] = jnp.where(mask, both[0], both[1]).astype(jnp.bfloat16)


def attn_bwd_kernel(q_ref, k_ref, v_ref, do_ref, dqkv_ref, dk_acc, dv_acc):
    seq_len = q_ref.shape[0]
    width = dqkv_ref.shape[1] // 3
    row0 = pl.multiple_of(pl.program_id(0) * seq_len, seq_len)
    col0 = pl.multiple_of(pl.program_id(1) * 2 * HEAD_DIM, 2 * HEAD_DIM)
    mask = head_mask(0)
    dk_acc[...] = jnp.zeros_like(dk_acc)
    dv_acc[...] = jnp.zeros_like(dv_acc)
    tn = (((0,), (0,)), ((), ()))
    for blk in range(seq_len // Q_BLOCK):
        rows = pl.ds(blk * Q_BLOCK, Q_BLOCK)
        n_key = (blk + 1) * Q_BLOCK
        both = []
        for which in range(2):
            hmask = head_mask(which)
            prob = block_probs(q_ref[rows, :], k_ref, blk, hmask)
            do_rows = do_ref[rows, :]
            do_one = jnp.where(hmask, do_rows, jnp.zeros_like(do_rows))
            q_rows = q_ref[rows, :]
            q_one = jnp.where(hmask, q_rows, jnp.zeros_like(q_rows))
            dprob = lax.dot_general(do_one, v_ref[:n_key, :], (((1,), (1,)), ((), ())), preferred_element_type=jnp.float32)
            inner = jnp.sum(prob * dprob, axis=-1, keepdims=True)
            dscore = (prob * (dprob - inner) * HEAD_DIM ** -0.5).astype(jnp.bfloat16)
            both.append(jnp.dot(dscore, k_ref[:n_key, :], preferred_element_type=jnp.float32))
            dk_acc[:n_key, :] += lax.dot_general(dscore, q_one, tn, preferred_element_type=jnp.float32)
            dv_acc[:n_key, :] += lax.dot_general(prob.astype(jnp.bfloat16), do_one, tn, preferred_element_type=jnp.float32)
        dqkv_ref[pl.ds(row0 + blk * Q_BLOCK, Q_BLOCK), pl.ds(col0, 2 * HEAD_DIM)] = jnp.where(mask, both[0], both[1]).astype(jnp.bfloat16)
    dqkv_ref[pl.ds(row0, seq_len), pl.ds(width + col0, 2 * HEAD_DIM)] = dk_acc[...].astype(jnp.bfloat16)
    dqkv_ref[pl.ds(row0, seq_len), pl.ds(2 * width + col0, 2 * HEAD_DIM)] = dv_acc[...].astype(jnp.bfloat16)


def head_specs(seq_len, n_pair):
    return [pl.BlockSpec((seq_len, 2 * HEAD_DIM), functools.partial(lambda part, b, h: (b, part * n_pair + h), part)) for part in range(3)]


def attention_forward(qkv_lo, n_batch, seq_len, width):
    n_pair = width // (2 * HEAD_DIM)
    n_tok = n_batch * seq_len
    return pl.pallas_call(
        attn_fwd_kernel,
        grid=(n_batch, n_pair),
        in_specs=head_specs(seq_len, n_pair),
        out_specs=pl.BlockSpec((seq_len, 2 * HEAD_DIM), lambda b, h: (b, h)),
        out_shape=jax.ShapeDtypeStruct((n_tok, width), jnp.bfloat16),
        cost_estimate=pl.CostEstimate(flops=14_000_000_000, bytes_accessed=6_300_000, transcendentals=4_700_000),
        compiler_params=pltpu.CompilerParams(dimension_semantics=("arbitrary", "arbitrary")),
        name="attn_fwd",
    )(qkv_lo, qkv_lo, qkv_lo)


def attention_backward(grad_attn, qkv_lo, n_batch, seq_len, width):
    n_pair = width // (2 * HEAD_DIM)
    n_tok = n_batch * seq_len
    return pl.pallas_call(
        attn_bwd_kernel,
        grid=(n_batch, n_pair),
        in_specs=head_specs(seq_len, n_pair) + [pl.BlockSpec((seq_len, 2 * HEAD_DIM), lambda b, h: (b, h))],
        out_specs=pl.BlockSpec((n_tok, 3 * width), lambda b, h: (0, 0)),
        out_shape=jax.ShapeDtypeStruct((n_tok, 3 * width), jnp.bfloat16),
        scratch_shapes=[pltpu.VMEM((seq_len, 2 * HEAD_DIM), jnp.float32)] * 2,
        cost_estimate=pl.CostEstimate(flops=40_000_000_000, bytes_accessed=12_600_000, transcendentals=4_700_000),
        compiler_params=pltpu.CompilerParams(dimension_semantics=("arbitrary", "arbitrary")),
        name="attn_bwd",
    )(qkv_lo, qkv_lo, qkv_lo, grad_attn)


def exchange(vals, mask):
    return lax.ppermute(vals, 'data', [(dev, dev ^ mask) for dev in range(N_DEV)])


N_BLOCK = 32
LAG = 2
SLOTS = 2 * LAG
BLOCK = 256
SQUARE = 1024
COLORS = ((2, 4, 8), (4, 8, 2), (8, 2, 4))
MESH_ID = pl.DeviceIdType.MESH


def reduce_kernel(*refs):
    (act_t, act_b, dy_t, dy_b, u2_t, u2_b, dz_t, dz_b, u1_t, u1_b, ao_t, ao_b, dqkv_t, dqkv_b, dh_t, dh_b,
     out_a, out_b, out_c, lhs_v, rhs_v, snd0, kp0, rcv0, snd1, kp1, rcv1, snd2, kp2, rcv2, snd3, kp3, rcv3, shard,
     load_sem, loc_sem, send_sem, recv_sem) = refs
    me = lax.axis_index('data')
    outs = (out_a, out_b, out_c)
    snds, kps, rcvs = (snd0, snd1, snd2, snd3), (kp0, kp1, kp2, kp3), (rcv0, rcv1, rcv2, rcv3)

    def bit(mask):
        return lax.rem(lax.div(me, mask), 2)

    def peer(mask):
        return me + mask * (1 - 2 * bit(mask))

    core = bit(1)
    barrier = pltpu.get_barrier_semaphore()
    for mask in (1, 2, 4, 8):
        pl.semaphore_signal(barrier, inc=1, device_id=(peer(mask),), device_id_type=MESH_ID)
    pl.semaphore_wait(barrier, 4)

    def place(blk):
        return lax.div(blk, 16), lax.div(lax.rem(blk, 16), 4), lax.rem(blk, 4)

    def region(k, blk, off, rows):
        top, sq, quarter = place(blk)
        layer = 1 - top
        row = quarter * BLOCK + off
        if k == 0:
            return outs[k].at[layer, pl.ds(pl.multiple_of(sq * SQUARE + row, 16), rows), :]
        return outs[k].at[layer, pl.ds(pl.multiple_of(row, 16), rows), pl.ds(pl.multiple_of(sq * SQUARE, SQUARE), SQUARE)]

    def load(k, blk, start):
        top, sq, quarter = place(blk)
        slot = lax.rem(blk, 2)
        dst_l, dst_r = lhs_v.at[k, slot], rhs_v.at[k, slot]

        def copies(lhs, rhs, lhs_col, rhs_col):
            return (pltpu.make_async_copy(lhs.at[:, pl.ds(pl.multiple_of(lhs_col, BLOCK), BLOCK)], dst_l, load_sem.at[k, slot, 0]),
                    pltpu.make_async_copy(rhs.at[:, pl.ds(pl.multiple_of(rhs_col, SQUARE), SQUARE)], dst_r, load_sem.at[k, slot, 1]))

        if not start:
            for copy in copies(u2_t, dz_t, 0, 0):
                copy.wait()
            return
        if k == 0:
            pairs = [(top == 0, act_t, dy_t, sq * SQUARE + quarter * BLOCK, 0), (top == 1, act_b, dy_b, sq * SQUARE + quarter * BLOCK, 0)]
        elif k == 1:
            pairs = [(top == 0, u2_t, dz_t, quarter * BLOCK, sq * SQUARE), (top == 1, u2_b, dz_b, quarter * BLOCK, sq * SQUARE)]
        else:
            pairs = [((top == 0) & (sq < 3), u1_t, dqkv_t, quarter * BLOCK, sq * SQUARE), ((top == 0) & (sq == 3), ao_t, dh_t, quarter * BLOCK, 0),
                     ((top == 1) & (sq < 3), u1_b, dqkv_b, quarter * BLOCK, sq * SQUARE), ((top == 1) & (sq == 3), ao_b, dh_b, quarter * BLOCK, 0)]
        for cond, lhs, rhs, lhs_col, rhs_col in pairs:
            @pl.when(cond)
            def _():
                for copy in copies(lhs, rhs, lhs_col, rhs_col):
                    copy.start()

    def remote(k, stage, slot, src, dst, mask):
        return pltpu.make_async_remote_copy(src_ref=src, dst_ref=dst, send_sem=send_sem.at[k, stage, slot], recv_sem=recv_sem.at[k, stage, slot],
                                            device_id=(peer(mask),), device_id_type=MESH_ID)

    def halves(k, stage, slot):
        mask = (1,) + COLORS[k]
        return remote(k, stage, slot, snds[stage].at[k, slot], rcvs[stage].at[k, slot], mask[stage])

    def offs(k):
        m1, m2, m3 = COLORS[k]
        b1, b2, b3 = bit(m1), bit(m2), bit(m3)
        base = core * 128
        return dict(own=base + b1 * 64 + b2 * 32 + b3 * 16, oth3=base + b1 * 64 + b2 * 32 + (1 - b3) * 16, pair=base + b1 * 64 + b2 * 32,
                    oth2=base + b1 * 64 + (1 - b2) * 32, quad=base + b1 * 64, oth1=base + (1 - b1) * 64)

    def gather(k, blk, slot, kind):
        o, (m1, m2, m3) = offs(k), COLORS[k]
        if kind == 'loc':
            return pltpu.make_async_copy(shard.at[k, slot], region(k, blk, o['own'], 16), loc_sem.at[k, slot])
        if kind == 't3':
            return remote(k, 4, slot, shard.at[k, slot], region(k, blk, o['own'], 16), m3)
        if kind == 'f0':
            return remote(k, 5, slot, shard.at[k, slot], region(k, blk, o['own'], 16), 1)
        name, rows, stage, mask = {'t2': ('pair', 32, 6, m2), 'f1': ('oth3', 16, 7, 1), 't1': ('quad', 64, 8, m1), 'f2': ('oth2', 32, 9, 1), 'f3': ('oth1', 64, 10, 1)}[kind]
        return remote(k, stage, slot, region(k, blk, o[name], rows), region(k, blk, o[name], rows), mask)

    starts = {4: ('loc', 't3', 'f0'), 5: ('t2', 'f1'), 6: ('t1', 'f2'), 7: ('f3',)}

    def wait_stage(k, stage, blk, slot):
        if stage == 0:
            load(k, blk, False)
            lslot = lax.rem(blk, 2)
            for half, dst in ((1 - core, snd0), (core, kp0)):
                lhs = lhs_v[k, lslot, :, pl.ds(pl.multiple_of(half * 128, 128), 128)]
                dst[k, slot] = lax.dot_general(lhs, rhs_v[k, lslot], (((0,), (0,)), ((), ())), preferred_element_type=jnp.float32)
        elif stage <= 4:
            halves(k, stage - 1, slot).wait()
            if stage == 4:
                shard[k, slot] = (kp3[k, slot] + rcv3[k, slot]) * (1.0 / N_DEV)
            else:
                rows = 128 >> stage
                side = bit(COLORS[k][stage - 1])
                keep, recv = kps[stage - 1], rcvs[stage - 1]
                for which, dst in ((1 - side, snds[stage]), (side, kps[stage])):
                    part = pl.ds(pl.multiple_of(which * rows, 16), rows)
                    dst[k, slot] = keep[k, slot, part, :] + recv[k, slot, part, :]
        else:
            for kind in starts[stage - 1]:
                gather(k, blk, slot, kind).wait()

    def start_stage(k, stage, blk, slot):
        if stage <= 3:
            halves(k, stage, slot).start()
        elif stage <= 7:
            for kind in starts[stage]:
                gather(k, blk, slot, kind).start()

    def step(t, _):
        for phase in (wait_stage, start_stage):
            for stage in range(9):
                blk = t - 1 - stage * LAG

                @pl.when((blk >= 0) & (blk < N_BLOCK))
                def _():
                    for k in range(3):
                        phase(k, stage, blk, lax.rem(blk, SLOTS))
            if phase is wait_stage:
                @pl.when(t < N_BLOCK)
                def _():
                    for k in range(3):
                        load(k, t, True)
        return 0

    lax.fori_loop(0, N_BLOCK + 1 + 8 * LAG, step, 0)


def reduce_gradients(pairs, n_layers, width, n_tok):
    shapes = [(n_layers, 4 * width, width), (n_layers, width, 4 * width), (n_layers, width, 4 * width)]
    f32 = jnp.float32

    def buf(rows):
        return pltpu.VMEM((3, SLOTS, rows, SQUARE), f32)

    scratch = [pltpu.VMEM((3, 2, n_tok, BLOCK), jnp.bfloat16), pltpu.VMEM((3, 2, n_tok, SQUARE), jnp.bfloat16)]
    for rows in (128, 64, 32, 16):
        scratch += [buf(rows)] * 3
    scratch += [buf(16), pltpu.SemaphoreType.DMA((3, 2, 2)), pltpu.SemaphoreType.DMA((3, SLOTS)),
                pltpu.SemaphoreType.DMA((3, 11, SLOTS)), pltpu.SemaphoreType.DMA((3, 11, SLOTS))]
    any_spec = pl.BlockSpec(memory_space=pl.ANY)
    return pl.pallas_call(
        reduce_kernel,
        out_shape=[jax.ShapeDtypeStruct(s, f32) for s in shapes],
        in_specs=[any_spec] * len(pairs),
        out_specs=[any_spec] * 3,
        scratch_shapes=scratch,
        cost_estimate=pl.CostEstimate(flops=600_000_000_000, bytes_accessed=400_000_000, transcendentals=0),
        compiler_params=pltpu.CompilerParams(collective_id=0, has_side_effects=True, vmem_limit_bytes=62 * 1024 * 1024),
        name="reduce_gradients",
    )(*pairs)


def add_small(vals):
    for mask in (1, 2, 4, 8):
        vals = vals + exchange(vals, mask)
    return vals * (1.0 / N_DEV)


def solution(mesh):
    def local_step(x_loc, grad_y_loc, gain_one, gain_two, w_qkv, w_out, w_up, w_down):
        n_layers, width = gain_one.shape
        n_batch, seq_len, _ = x_loc.shape
        x_blk = x_loc.reshape(n_batch * seq_len, width)
        saved_all = []
        for layer_idx in range(n_layers):
            norm_a, norm_a_back = jax.vjp(rms_gain, x_blk.astype(jnp.float32), gain_one[layer_idx])
            u_one = norm_a.astype(jnp.bfloat16)
            qkv_lo = dot_lo(u_one, w_qkv[layer_idx])
            attn_out = attention_forward(qkv_lo, n_batch, seq_len, width)
            hidden = x_blk + dot_lo(attn_out, w_out[layer_idx])
            norm_b, norm_b_back = jax.vjp(rms_gain, hidden.astype(jnp.float32), gain_two[layer_idx])
            u_two = norm_b.astype(jnp.bfloat16)
            pre_lo = dot_lo(u_two, w_up[layer_idx])
            act_f, gelu_back = jax.vjp(gelu_tanh, pre_lo.astype(jnp.float32))
            act_lo = act_f.astype(jnp.bfloat16)
            saved_all.append((norm_a_back, u_one, qkv_lo, attn_out, norm_b_back, u_two, gelu_back, act_lo))
            if layer_idx + 1 < n_layers:
                x_blk = hidden + dot_lo(act_lo, w_down[layer_idx])
        grad_cur = grad_y_loc.reshape(n_batch * seq_len, width)
        gains = [None] * n_layers
        pairs = []
        for layer_idx in reversed(range(n_layers)):
            norm_a_back, u_one, qkv_lo, attn_out, norm_b_back, u_two, gelu_back, act_lo = saved_all[layer_idx]
            grad_top = grad_cur
            grad_act = dot_nt(grad_cur, w_down[layer_idx])
            (grad_pre_f,) = gelu_back(grad_act.astype(jnp.float32))
            grad_pre = grad_pre_f.astype(jnp.bfloat16)
            grad_u_two = dot_nt(grad_pre, w_up[layer_idx])
            grad_h_norm, grad_gain_b = norm_b_back(grad_u_two.astype(jnp.float32))
            grad_hidden = (grad_cur.astype(jnp.float32) + grad_h_norm).astype(jnp.bfloat16)
            grad_attn = dot_nt(grad_hidden, w_out[layer_idx])
            grad_qkv = attention_backward(grad_attn, qkv_lo, n_batch, seq_len, width)
            grad_u_one = dot_nt(grad_qkv, w_qkv[layer_idx])
            grad_x_norm, grad_gain_a = norm_a_back(grad_u_one.astype(jnp.float32))
            grad_cur = (grad_hidden.astype(jnp.float32) + grad_x_norm).astype(jnp.bfloat16)
            gains[layer_idx] = (grad_gain_a, grad_gain_b)
            pairs.append((act_lo, grad_top, u_two, grad_pre, u_one, attn_out, grad_qkv, grad_hidden))
        small = add_small(jnp.stack([g[0] for g in gains] + [g[1] for g in gains]))
        flat = [val for both in zip(*pairs) for val in both]
        sum_down, sum_up, sum_attn = reduce_gradients(flat, n_layers, width, n_batch * seq_len)
        return grad_cur.reshape(x_loc.shape), small[:n_layers], small[n_layers:], sum_attn[:, :, :3 * width], sum_attn[:, :, 3 * width:], sum_up, sum_down

    batch_spec = P('data')
    full_spec = P()
    return jax.shard_map(local_step, mesh=mesh, in_specs=(batch_spec, batch_spec) + (full_spec,) * 6, out_specs=(batch_spec,) + (full_spec,) * 6, check_vma=False)
```

```python
import functools

import jax
import jax.numpy as jnp
from jax import lax
from jax.experimental import pallas as pl
from jax.experimental.pallas import tpu as pltpu
from jax.sharding import PartitionSpec as P

NORM_EPS = 1e-6
HEAD_DIM = 64
N_DEV = 16


def rms_gain(rows_f, gain_vec):
    return rows_f * lax.rsqrt(jnp.mean(rows_f * rows_f, axis=-1, keepdims=True) + NORM_EPS) * gain_vec


def gelu_tanh(pre_act):
    return jax.nn.gelu(pre_act, approximate=True)


def dot_lo(lhs, rhs):
    return lax.dot_general(lhs, rhs, (((1,), (0,)), ((), ())), preferred_element_type=jnp.float32).astype(jnp.bfloat16)


def dot_nt(lhs, rhs):
    return lax.dot_general(lhs, rhs, (((1,), (1,)), ((), ())), preferred_element_type=jnp.float32).astype(jnp.bfloat16)


def dot_tn(lhs, rhs):
    return lax.dot_general(lhs, rhs, (((0,), (0,)), ((), ())), preferred_element_type=jnp.float32)


PAIR = 2 * HEAD_DIM
PAIRS_PER_STEP = 2


def head_mask(which, seq_len):
    lane = lax.broadcasted_iota(jnp.int32, (seq_len, PAIR), 1)
    return (lane >= which * HEAD_DIM) & (lane < (which + 1) * HEAD_DIM)


def one_head(rows, which):
    return jnp.where(head_mask(which, rows.shape[0]), rows, jnp.zeros_like(rows))


def head_probs(q_one, k_rows):
    seq_len = q_one.shape[0]
    scores = lax.dot_general(q_one, k_rows, (((1,), (1,)), ((), ())), preferred_element_type=jnp.float32) * HEAD_DIM ** -0.5
    row = lax.broadcasted_iota(jnp.int32, (seq_len, seq_len), 0)
    col = lax.broadcasted_iota(jnp.int32, (seq_len, seq_len), 1)
    scores = jnp.where(row >= col, scores, -1e30)
    expo = jnp.exp(scores - jnp.max(scores, axis=-1, keepdims=True))
    return expo * (1.0 / jnp.sum(expo, axis=-1, keepdims=True))


def pair_backward(q_rows, k_rows, v_rows, do_rows):
    tn = (((0,), (0,)), ((), ()))
    grads = []
    for which in range(2):
        q_one, do_one = one_head(q_rows, which), one_head(do_rows, which)
        prob = head_probs(q_one, k_rows)
        dprob = lax.dot_general(do_one, v_rows, (((1,), (1,)), ((), ())), preferred_element_type=jnp.float32)
        inner = jnp.sum(prob * dprob, axis=-1, keepdims=True)
        dscore = (prob * (dprob - inner) * HEAD_DIM ** -0.5).astype(jnp.bfloat16)
        dq = jnp.dot(dscore, k_rows, preferred_element_type=jnp.float32)
        dk = lax.dot_general(dscore, q_one, tn, preferred_element_type=jnp.float32)
        dv = lax.dot_general(prob.astype(jnp.bfloat16), do_one, tn, preferred_element_type=jnp.float32)
        grads.append((dq, dk, dv))
    mask = head_mask(0, q_rows.shape[0])
    return [jnp.where(mask, one, two).astype(jnp.bfloat16) for one, two in zip(*grads)]


def attn_fwd_kernel(q_ref, k_ref, v_ref, o_ref):
    mask = head_mask(0, q_ref.shape[0])
    for pair in range(PAIRS_PER_STEP):
        cols = pl.ds(pair * PAIR, PAIR)
        both = []
        for which in range(2):
            prob = head_probs(one_head(q_ref[:, cols], which), k_ref[:, cols]).astype(jnp.bfloat16)
            both.append(jnp.dot(prob, v_ref[:, cols], preferred_element_type=jnp.float32))
        o_ref[:, cols] = jnp.where(mask, both[0], both[1]).astype(jnp.bfloat16)


def attn_bwd_kernel(q_ref, k_ref, v_ref, do_ref, dqkv_ref):
    seq_len = q_ref.shape[0]
    width = dqkv_ref.shape[1] // 3
    row0 = pl.multiple_of(pl.program_id(0) * seq_len, seq_len)
    for pair in range(PAIRS_PER_STEP):
        cols = pl.ds(pair * PAIR, PAIR)
        col0 = pl.multiple_of((pl.program_id(1) * PAIRS_PER_STEP + pair) * PAIR, PAIR)
        grads = pair_backward(q_ref[:, cols], k_ref[:, cols], v_ref[:, cols], do_ref[:, cols])
        for part, vals in enumerate(grads):
            dqkv_ref[pl.ds(row0, seq_len), pl.ds(part * width + col0, PAIR)] = vals


def head_specs(seq_len, n_step, lanes):
    return [pl.BlockSpec((seq_len, lanes), functools.partial(lambda part, b, h: (b, part * n_step + h), part)) for part in range(3)]


def attention_forward(qkv_lo, n_batch, seq_len, width):
    lanes = PAIR * PAIRS_PER_STEP
    n_step = width // lanes
    n_tok = n_batch * seq_len
    return pl.pallas_call(
        attn_fwd_kernel,
        grid=(n_batch, n_step),
        in_specs=head_specs(seq_len, n_step, lanes),
        out_specs=pl.BlockSpec((seq_len, lanes), lambda b, h: (b, h)),
        out_shape=jax.ShapeDtypeStruct((n_tok, width), jnp.bfloat16),
        cost_estimate=pl.CostEstimate(flops=14_000_000_000, bytes_accessed=6_300_000, transcendentals=4_700_000),
        compiler_params=pltpu.CompilerParams(dimension_semantics=("arbitrary", "arbitrary")),
        name="attn_fwd",
    )(qkv_lo, qkv_lo, qkv_lo)


def attention_backward(grad_attn, qkv_lo, n_batch, seq_len, width):
    lanes = PAIR * PAIRS_PER_STEP
    n_step = width // lanes
    n_tok = n_batch * seq_len
    return pl.pallas_call(
        attn_bwd_kernel,
        grid=(n_batch, n_step),
        in_specs=head_specs(seq_len, n_step, lanes) + [pl.BlockSpec((seq_len, lanes), lambda b, h: (b, h))],
        out_specs=pl.BlockSpec((n_tok, 3 * width), lambda b, h: (0, 0)),
        out_shape=jax.ShapeDtypeStruct((n_tok, 3 * width), jnp.bfloat16),
        cost_estimate=pl.CostEstimate(flops=40_000_000_000, bytes_accessed=12_600_000, transcendentals=4_700_000),
        compiler_params=pltpu.CompilerParams(dimension_semantics=("arbitrary", "arbitrary")),
        name="attn_bwd",
    )(qkv_lo, qkv_lo, qkv_lo, grad_attn)


def exchange(vals, mask):
    return lax.ppermute(vals, 'data', [(dev, dev ^ mask) for dev in range(N_DEV)])


N_BLOCK = 32
LAG = 2
SLOTS = 2 * LAG
BLOCK = 256
SQUARE = 1024
COLORS = ((2, 4, 8), (4, 8, 2), (8, 2, 4))
MESH_ID = pl.DeviceIdType.MESH


def reduce_kernel(*refs):
    (act_t, act_b, dy_t, dy_b, u2_t, u2_b, dz_t, dz_b, u1_t, u1_b, ao_t, ao_b, dqkv_t, dqkv_b, dh_t, dh_b,
     out_a, out_b, out_c, lhs_v, rhs_v, snd0, kp0, rcv0, snd1, kp1, rcv1, snd2, kp2, rcv2, snd3, kp3, rcv3, shard,
     load_sem, loc_sem, send_sem, recv_sem) = refs
    me = lax.axis_index('data')
    outs = (out_a, out_b, out_c)
    snds, kps, rcvs = (snd0, snd1, snd2, snd3), (kp0, kp1, kp2, kp3), (rcv0, rcv1, rcv2, rcv3)

    def bit(mask):
        return lax.rem(lax.div(me, mask), 2)

    def peer(mask):
        return me + mask * (1 - 2 * bit(mask))

    core = bit(1)
    barrier = pltpu.get_barrier_semaphore()
    for mask in (1, 2, 4, 8):
        pl.semaphore_signal(barrier, inc=1, device_id=(peer(mask),), device_id_type=MESH_ID)
    pl.semaphore_wait(barrier, 4)

    def place(blk):
        return lax.div(blk, 16), lax.div(lax.rem(blk, 16), 4), lax.rem(blk, 4)

    def region(k, blk, off, rows):
        top, sq, quarter = place(blk)
        layer = 1 - top
        row = quarter * BLOCK + off
        if k == 0:
            return outs[k].at[layer, pl.ds(pl.multiple_of(sq * SQUARE + row, 16), rows), :]
        return outs[k].at[layer, pl.ds(pl.multiple_of(row, 16), rows), pl.ds(pl.multiple_of(sq * SQUARE, SQUARE), SQUARE)]

    def load(k, blk, start):
        top, sq, quarter = place(blk)
        slot = lax.rem(blk, 2)
        dst_l, dst_r = lhs_v.at[k, slot], rhs_v.at[k, slot]

        def copies(lhs, rhs, lhs_col, rhs_col):
            return (pltpu.make_async_copy(lhs.at[:, pl.ds(pl.multiple_of(lhs_col, BLOCK), BLOCK)], dst_l, load_sem.at[k, slot, 0]),
                    pltpu.make_async_copy(rhs.at[:, pl.ds(pl.multiple_of(rhs_col, SQUARE), SQUARE)], dst_r, load_sem.at[k, slot, 1]))

        if not start:
            for copy in copies(u2_t, dz_t, 0, 0):
                copy.wait()
            return
        if k == 0:
            pairs = [(top == 0, act_t, dy_t, sq * SQUARE + quarter * BLOCK, 0), (top == 1, act_b, dy_b, sq * SQUARE + quarter * BLOCK, 0)]
        elif k == 1:
            pairs = [(top == 0, u2_t, dz_t, quarter * BLOCK, sq * SQUARE), (top == 1, u2_b, dz_b, quarter * BLOCK, sq * SQUARE)]
        else:
            pairs = [((top == 0) & (sq < 3), u1_t, dqkv_t, quarter * BLOCK, sq * SQUARE), ((top == 0) & (sq == 3), ao_t, dh_t, quarter * BLOCK, 0),
                     ((top == 1) & (sq < 3), u1_b, dqkv_b, quarter * BLOCK, sq * SQUARE), ((top == 1) & (sq == 3), ao_b, dh_b, quarter * BLOCK, 0)]
        for cond, lhs, rhs, lhs_col, rhs_col in pairs:
            @pl.when(cond)
            def _():
                for copy in copies(lhs, rhs, lhs_col, rhs_col):
                    copy.start()

    def remote(k, stage, slot, src, dst, mask):
        return pltpu.make_async_remote_copy(src_ref=src, dst_ref=dst, send_sem=send_sem.at[k, stage, slot], recv_sem=recv_sem.at[k, stage, slot],
                                            device_id=(peer(mask),), device_id_type=MESH_ID)

    def halves(k, stage, slot):
        mask = (1,) + COLORS[k]
        return remote(k, stage, slot, snds[stage].at[k, slot], rcvs[stage].at[k, slot], mask[stage])

    def offs(k):
        m1, m2, m3 = COLORS[k]
        b1, b2, b3 = bit(m1), bit(m2), bit(m3)
        base = core * 128
        return dict(own=base + b1 * 64 + b2 * 32 + b3 * 16, oth3=base + b1 * 64 + b2 * 32 + (1 - b3) * 16, pair=base + b1 * 64 + b2 * 32,
                    oth2=base + b1 * 64 + (1 - b2) * 32, quad=base + b1 * 64, oth1=base + (1 - b1) * 64)

    def gather(k, blk, slot, kind):
        o, (m1, m2, m3) = offs(k), COLORS[k]
        if kind == 'loc':
            return pltpu.make_async_copy(shard.at[k, slot], region(k, blk, o['own'], 16), loc_sem.at[k, slot])
        if kind == 't3':
            return remote(k, 4, slot, shard.at[k, slot], region(k, blk, o['own'], 16), m3)
        if kind == 'f0':
            return remote(k, 5, slot, shard.at[k, slot], region(k, blk, o['own'], 16), 1)
        name, rows, stage, mask = {'t2': ('pair', 32, 6, m2), 'f1': ('oth3', 16, 7, 1), 't1': ('quad', 64, 8, m1), 'f2': ('oth2', 32, 9, 1), 'f3': ('oth1', 64, 10, 1)}[kind]
        return remote(k, stage, slot, region(k, blk, o[name], rows), region(k, blk, o[name], rows), mask)

    starts = {4: ('loc', 't3', 'f0'), 5: ('t2', 'f1'), 6: ('t1', 'f2'), 7: ('f3',)}

    def wait_stage(k, stage, blk, slot):
        if stage == 0:
            load(k, blk, False)
            lslot = lax.rem(blk, 2)
            for half, dst in ((1 - core, snd0), (core, kp0)):
                lhs = lhs_v[k, lslot, :, pl.ds(pl.multiple_of(half * 128, 128), 128)]
                dst[k, slot] = lax.dot_general(lhs, rhs_v[k, lslot], (((0,), (0,)), ((), ())), preferred_element_type=jnp.float32)
        elif stage <= 4:
            halves(k, stage - 1, slot).wait()
            if stage == 4:
                shard[k, slot] = (kp3[k, slot] + rcv3[k, slot]) * (1.0 / N_DEV)
            else:
                rows = 128 >> stage
                side = bit(COLORS[k][stage - 1])
                keep, recv = kps[stage - 1], rcvs[stage - 1]
                for which, dst in ((1 - side, snds[stage]), (side, kps[stage])):
                    part = pl.ds(pl.multiple_of(which * rows, 16), rows)
                    dst[k, slot] = keep[k, slot, part, :] + recv[k, slot, part, :]
        else:
            for kind in starts[stage - 1]:
                gather(k, blk, slot, kind).wait()

    def start_stage(k, stage, blk, slot):
        if stage <= 3:
            halves(k, stage, slot).start()
        elif stage <= 7:
            for kind in starts[stage]:
                gather(k, blk, slot, kind).start()

    def step(t, _):
        for phase in (wait_stage, start_stage):
            for stage in range(9):
                blk = t - 1 - stage * LAG

                @pl.when((blk >= 0) & (blk < N_BLOCK))
                def _():
                    for k in range(3):
                        phase(k, stage, blk, lax.rem(blk, SLOTS))
            if phase is wait_stage:
                @pl.when(t < N_BLOCK)
                def _():
                    for k in range(3):
                        load(k, t, True)
        return 0

    lax.fori_loop(0, N_BLOCK + 1 + 8 * LAG, step, 0)


def reduce_gradients(pairs, n_layers, width, n_tok):
    shapes = [(n_layers, 4 * width, width), (n_layers, width, 4 * width), (n_layers, width, 4 * width)]
    f32 = jnp.float32

    def buf(rows):
        return pltpu.VMEM((3, SLOTS, rows, SQUARE), f32)

    scratch = [pltpu.VMEM((3, 2, n_tok, BLOCK), jnp.bfloat16), pltpu.VMEM((3, 2, n_tok, SQUARE), jnp.bfloat16)]
    for rows in (128, 64, 32, 16):
        scratch += [buf(rows)] * 3
    scratch += [buf(16), pltpu.SemaphoreType.DMA((3, 2, 2)), pltpu.SemaphoreType.DMA((3, SLOTS)),
                pltpu.SemaphoreType.DMA((3, 11, SLOTS)), pltpu.SemaphoreType.DMA((3, 11, SLOTS))]
    any_spec = pl.BlockSpec(memory_space=pl.ANY)
    return pl.pallas_call(
        reduce_kernel,
        out_shape=[jax.ShapeDtypeStruct(s, f32) for s in shapes],
        in_specs=[any_spec] * len(pairs),
        out_specs=[any_spec] * 3,
        scratch_shapes=scratch,
        cost_estimate=pl.CostEstimate(flops=600_000_000_000, bytes_accessed=400_000_000, transcendentals=0),
        compiler_params=pltpu.CompilerParams(collective_id=0, has_side_effects=True, vmem_limit_bytes=62 * 1024 * 1024),
        name="reduce_gradients",
    )(*pairs)


def add_small(vals):
    for mask in (1, 2, 4, 8):
        vals = vals + exchange(vals, mask)
    return vals * (1.0 / N_DEV)


def solution(mesh):
    def local_step(x_loc, grad_y_loc, gain_one, gain_two, w_qkv, w_out, w_up, w_down):
        n_layers, width = gain_one.shape
        n_batch, seq_len, _ = x_loc.shape
        x_blk = x_loc.reshape(n_batch * seq_len, width)
        saved_all = []
        for layer_idx in range(n_layers):
            norm_a, norm_a_back = jax.vjp(rms_gain, x_blk.astype(jnp.float32), gain_one[layer_idx])
            u_one = norm_a.astype(jnp.bfloat16)
            qkv_lo = dot_lo(u_one, w_qkv[layer_idx])
            attn_out = attention_forward(qkv_lo, n_batch, seq_len, width)
            hidden = x_blk + dot_lo(attn_out, w_out[layer_idx])
            norm_b, norm_b_back = jax.vjp(rms_gain, hidden.astype(jnp.float32), gain_two[layer_idx])
            u_two = norm_b.astype(jnp.bfloat16)
            pre_lo = dot_lo(u_two, w_up[layer_idx])
            act_f, gelu_back = jax.vjp(gelu_tanh, pre_lo.astype(jnp.float32))
            act_lo = act_f.astype(jnp.bfloat16)
            saved_all.append((norm_a_back, u_one, qkv_lo, attn_out, norm_b_back, u_two, gelu_back, act_lo))
            if layer_idx + 1 < n_layers:
                x_blk = hidden + dot_lo(act_lo, w_down[layer_idx])
        grad_cur = grad_y_loc.reshape(n_batch * seq_len, width)
        gains = [None] * n_layers
        pairs = []
        for layer_idx in reversed(range(n_layers)):
            norm_a_back, u_one, qkv_lo, attn_out, norm_b_back, u_two, gelu_back, act_lo = saved_all[layer_idx]
            grad_top = grad_cur
            grad_act = dot_nt(grad_cur, w_down[layer_idx])
            (grad_pre_f,) = gelu_back(grad_act.astype(jnp.float32))
            grad_pre = grad_pre_f.astype(jnp.bfloat16)
            grad_u_two = dot_nt(grad_pre, w_up[layer_idx])
            grad_h_norm, grad_gain_b = norm_b_back(grad_u_two.astype(jnp.float32))
            grad_hidden = (grad_cur.astype(jnp.float32) + grad_h_norm).astype(jnp.bfloat16)
            grad_attn = dot_nt(grad_hidden, w_out[layer_idx])
            grad_qkv = attention_backward(grad_attn, qkv_lo, n_batch, seq_len, width)
            grad_u_one = dot_nt(grad_qkv, w_qkv[layer_idx])
            grad_x_norm, grad_gain_a = norm_a_back(grad_u_one.astype(jnp.float32))
            grad_cur = (grad_hidden.astype(jnp.float32) + grad_x_norm).astype(jnp.bfloat16)
            gains[layer_idx] = (grad_gain_a, grad_gain_b)
            pairs.append((act_lo, grad_top, u_two, grad_pre, u_one, attn_out, grad_qkv, grad_hidden))
        small = add_small(jnp.stack([g[0] for g in gains] + [g[1] for g in gains]))
        flat = [val for both in zip(*pairs) for val in both]
        sum_down, sum_up, sum_attn = reduce_gradients(flat, n_layers, width, n_batch * seq_len)
        return grad_cur.reshape(x_loc.shape), small[:n_layers], small[n_layers:], sum_attn[:, :, :3 * width], sum_attn[:, :, 3 * width:], sum_up, sum_down

    batch_spec = P('data')
    full_spec = P()
    return jax.shard_map(local_step, mesh=mesh, in_specs=(batch_spec, batch_spec) + (full_spec,) * 6, out_specs=(batch_spec,) + (full_spec,) * 6, check_vma=False)
```

```python
import functools

import jax
import jax.numpy as jnp
from jax import lax
from jax.experimental import pallas as pl
from jax.experimental.pallas import tpu as pltpu
from jax.sharding import PartitionSpec as P

NORM_EPS = 1e-6
GELU_C = 0.7978845608028654
HEAD_DIM = 64
N_DEV = 16


def rms_gain(rows_f, gain_vec):
    return rows_f * lax.rsqrt(jnp.mean(rows_f * rows_f, axis=-1, keepdims=True) + NORM_EPS) * gain_vec


def gelu_tanh(pre_act):
    return jax.nn.gelu(pre_act, approximate=True)


def dot_lo(lhs, rhs):
    return lax.dot_general(lhs, rhs, (((1,), (0,)), ((), ())), preferred_element_type=jnp.float32).astype(jnp.bfloat16)


def dot_nt(lhs, rhs):
    return lax.dot_general(lhs, rhs, (((1,), (1,)), ((), ())), preferred_element_type=jnp.float32).astype(jnp.bfloat16)


def dot_tn(lhs, rhs):
    return lax.dot_general(lhs, rhs, (((0,), (0,)), ((), ())), preferred_element_type=jnp.float32)


PAIR = 2 * HEAD_DIM
PAIRS_PER_STEP = 2


def head_mask(which, seq_len):
    lane = lax.broadcasted_iota(jnp.int32, (seq_len, PAIR), 1)
    return (lane >= which * HEAD_DIM) & (lane < (which + 1) * HEAD_DIM)


def one_head(rows, which):
    return jnp.where(head_mask(which, rows.shape[0]), rows, jnp.zeros_like(rows))


def head_probs(q_one, k_rows):
    seq_len = q_one.shape[0]
    scores = lax.dot_general(q_one, k_rows, (((1,), (1,)), ((), ())), preferred_element_type=jnp.float32) * HEAD_DIM ** -0.5
    row = lax.broadcasted_iota(jnp.int32, (seq_len, seq_len), 0)
    col = lax.broadcasted_iota(jnp.int32, (seq_len, seq_len), 1)
    scores = jnp.where(row >= col, scores, -1e30)
    expo = jnp.exp(scores - jnp.max(scores, axis=-1, keepdims=True))
    return expo * (1.0 / jnp.sum(expo, axis=-1, keepdims=True))


def pair_backward(q_rows, k_rows, v_rows, do_rows):
    tn = (((0,), (0,)), ((), ()))
    grads = []
    for which in range(2):
        q_one, do_one = one_head(q_rows, which), one_head(do_rows, which)
        prob = head_probs(q_one, k_rows)
        dprob = lax.dot_general(do_one, v_rows, (((1,), (1,)), ((), ())), preferred_element_type=jnp.float32)
        inner = jnp.sum(prob * dprob, axis=-1, keepdims=True)
        dscore = (prob * (dprob - inner) * HEAD_DIM ** -0.5).astype(jnp.bfloat16)
        dq = jnp.dot(dscore, k_rows, preferred_element_type=jnp.float32)
        dk = lax.dot_general(dscore, q_one, tn, preferred_element_type=jnp.float32)
        dv = lax.dot_general(prob.astype(jnp.bfloat16), do_one, tn, preferred_element_type=jnp.float32)
        grads.append((dq, dk, dv))
    mask = head_mask(0, q_rows.shape[0])
    return [jnp.where(mask, one, two).astype(jnp.bfloat16) for one, two in zip(*grads)]


def attn_fwd_kernel(q_ref, k_ref, v_ref, o_ref):
    mask = head_mask(0, q_ref.shape[0])
    for pair in range(PAIRS_PER_STEP):
        cols = pl.ds(pair * PAIR, PAIR)
        both = []
        for which in range(2):
            prob = head_probs(one_head(q_ref[:, cols], which), k_ref[:, cols]).astype(jnp.bfloat16)
            both.append(jnp.dot(prob, v_ref[:, cols], preferred_element_type=jnp.float32))
        o_ref[:, cols] = jnp.where(mask, both[0], both[1]).astype(jnp.bfloat16)


def attn_bwd_kernel(q_ref, k_ref, v_ref, do_ref, dqkv_ref):
    seq_len = q_ref.shape[0]
    width = dqkv_ref.shape[1] // 3
    row0 = pl.multiple_of(pl.program_id(0) * seq_len, seq_len)
    for pair in range(PAIRS_PER_STEP):
        cols = pl.ds(pair * PAIR, PAIR)
        col0 = pl.multiple_of((pl.program_id(1) * PAIRS_PER_STEP + pair) * PAIR, PAIR)
        grads = pair_backward(q_ref[:, cols], k_ref[:, cols], v_ref[:, cols], do_ref[:, cols])
        for part, vals in enumerate(grads):
            dqkv_ref[pl.ds(row0, seq_len), pl.ds(part * width + col0, PAIR)] = vals


def head_specs(seq_len, n_step, lanes):
    return [pl.BlockSpec((seq_len, lanes), functools.partial(lambda part, b, h: (b, part * n_step + h), part)) for part in range(3)]


def attention_forward(qkv_lo, n_batch, seq_len, width):
    lanes = PAIR * PAIRS_PER_STEP
    n_step = width // lanes
    n_tok = n_batch * seq_len
    return pl.pallas_call(
        attn_fwd_kernel,
        grid=(n_batch, n_step),
        in_specs=head_specs(seq_len, n_step, lanes),
        out_specs=pl.BlockSpec((seq_len, lanes), lambda b, h: (b, h)),
        out_shape=jax.ShapeDtypeStruct((n_tok, width), jnp.bfloat16),
        cost_estimate=pl.CostEstimate(flops=14_000_000_000, bytes_accessed=6_300_000, transcendentals=4_700_000),
        compiler_params=pltpu.CompilerParams(dimension_semantics=("arbitrary", "arbitrary")),
        name="attn_fwd",
    )(qkv_lo, qkv_lo, qkv_lo)


def attention_backward(grad_attn, qkv_lo, n_batch, seq_len, width):
    lanes = PAIR * PAIRS_PER_STEP
    n_step = width // lanes
    n_tok = n_batch * seq_len
    return pl.pallas_call(
        attn_bwd_kernel,
        grid=(n_batch, n_step),
        in_specs=head_specs(seq_len, n_step, lanes) + [pl.BlockSpec((seq_len, lanes), lambda b, h: (b, h))],
        out_specs=pl.BlockSpec((n_tok, 3 * width), lambda b, h: (0, 0)),
        out_shape=jax.ShapeDtypeStruct((n_tok, 3 * width), jnp.bfloat16),
        cost_estimate=pl.CostEstimate(flops=40_000_000_000, bytes_accessed=12_600_000, transcendentals=4_700_000),
        compiler_params=pltpu.CompilerParams(dimension_semantics=("arbitrary", "arbitrary")),
        name="attn_bwd",
    )(qkv_lo, qkv_lo, qkv_lo, grad_attn)


def exchange(vals, mask):
    return lax.ppermute(vals, 'data', [(dev, dev ^ mask) for dev in range(N_DEV)])


N_BLOCK = 32
LAG = 2
SLOTS = 2 * LAG
OWN_SLOTS = LAG + 1
TILE = 256
N_TILE_STEP = 8
UNITS = 3
BLOCK = 256
SQUARE = 1024
COLORS = ((2, 4, 8), (4, 8, 2), (8, 2, 4))
MESH_ID = pl.DeviceIdType.MESH


def reduce_kernel(*refs):
    (act_t, act_b, dy_t, dy_b, u2_t, u2_b, dz_t, u1_t, u1_b, ao_t, ao_b, dqkv_t, dh_t, pre_b, hid_b, qkv_b, w_down, w_up, w_out, gain_ref,
     out_a, out_b, out_c, dz_b, dh_b, dqkv_b, dgain_ref, lhs_v, rhs_v, snd0, kp0, rcv0, snd1, kp1, rcv1, snd2, kp2, rcv2, snd3, kp3, rcv3, shard,
     dy_v, hid_v, acc_v, w2_v, w1_v, z_v, dz_v, wo_v, qkv_v, dqkv_v,
     load_sem, loc_sem, send_sem, recv_sem, whole_sem, tile_sem, head_sem, put_sem) = refs
    me = lax.axis_index('data')
    outs = (out_a, out_b, out_c)
    snds, kps, rcvs = (snd0, snd1, snd2, snd3), (kp0, kp1, kp2, kp3), (rcv0, rcv1, rcv2, rcv3)

    def bit(mask):
        return lax.rem(lax.div(me, mask), 2)

    def peer(mask):
        return me + mask * (1 - 2 * bit(mask))

    core = bit(1)
    barrier = pltpu.get_barrier_semaphore()
    for mask in (1, 2, 4, 8):
        pl.semaphore_signal(barrier, inc=1, device_id=(peer(mask),), device_id_type=MESH_ID)
    pl.semaphore_wait(barrier, 4)

    def place(blk):
        return lax.div(blk, 16), lax.div(lax.rem(blk, 16), 4), lax.rem(blk, 4)

    def region(k, blk, off, rows):
        top, sq, quarter = place(blk)
        layer = 1 - top
        row = quarter * BLOCK + off
        if k == 0:
            return outs[k].at[layer, pl.ds(pl.multiple_of(sq * SQUARE + row, 16), rows), :]
        return outs[k].at[layer, pl.ds(pl.multiple_of(row, 16), rows), pl.ds(pl.multiple_of(sq * SQUARE, SQUARE), SQUARE)]

    def load(k, blk, start):
        top, sq, quarter = place(blk)
        slot = lax.rem(blk, 2)
        dst_l, dst_r = lhs_v.at[k, slot], rhs_v.at[k, slot]

        def copies(lhs, rhs, lhs_col, rhs_col):
            return (pltpu.make_async_copy(lhs.at[:, pl.ds(pl.multiple_of(lhs_col, BLOCK), BLOCK)], dst_l, load_sem.at[k, slot, 0]),
                    pltpu.make_async_copy(rhs.at[:, pl.ds(pl.multiple_of(rhs_col, SQUARE), SQUARE)], dst_r, load_sem.at[k, slot, 1]))

        if not start:
            for copy in copies(u2_t, dz_t, 0, 0):
                copy.wait()
            return
        if k == 0:
            pairs = [(top == 0, act_t, dy_t, sq * SQUARE + quarter * BLOCK, 0), (top == 1, act_b, dy_b, sq * SQUARE + quarter * BLOCK, 0)]
        elif k == 1:
            pairs = [(top == 0, u2_t, dz_t, quarter * BLOCK, sq * SQUARE), (top == 1, u2_b, dz_b, quarter * BLOCK, sq * SQUARE)]
        else:
            pairs = [((top == 0) & (sq < 3), u1_t, dqkv_t, quarter * BLOCK, sq * SQUARE), ((top == 0) & (sq == 3), ao_t, dh_t, quarter * BLOCK, 0),
                     ((top == 1) & (sq < 3), u1_b, dqkv_b, quarter * BLOCK, sq * SQUARE), ((top == 1) & (sq == 3), ao_b, dh_b, quarter * BLOCK, 0)]
        for cond, lhs, rhs, lhs_col, rhs_col in pairs:
            @pl.when(cond)
            def _():
                for copy in copies(lhs, rhs, lhs_col, rhs_col):
                    copy.start()

    def remote(k, stage, slot, src, dst, mask):
        return pltpu.make_async_remote_copy(src_ref=src, dst_ref=dst, send_sem=send_sem.at[k, stage, slot], recv_sem=recv_sem.at[k, stage, slot],
                                            device_id=(peer(mask),), device_id_type=MESH_ID)

    def halves(k, stage, slot, own):
        mask = (1,) + COLORS[k]
        return remote(k, stage, slot, snds[stage].at[k, own], rcvs[stage].at[k, slot], mask[stage])

    def offs(k):
        m1, m2, m3 = COLORS[k]
        b1, b2, b3 = bit(m1), bit(m2), bit(m3)
        base = core * 128
        return dict(own=base + b1 * 64 + b2 * 32 + b3 * 16, oth3=base + b1 * 64 + b2 * 32 + (1 - b3) * 16, pair=base + b1 * 64 + b2 * 32,
                    oth2=base + b1 * 64 + (1 - b2) * 32, quad=base + b1 * 64, oth1=base + (1 - b1) * 64)

    def gather(k, blk, slot, kind):
        o, (m1, m2, m3) = offs(k), COLORS[k]
        if kind == 'loc':
            return pltpu.make_async_copy(shard.at[k, slot], region(k, blk, o['own'], 16), loc_sem.at[k, slot])
        if kind == 't3':
            return remote(k, 4, slot, shard.at[k, slot], region(k, blk, o['own'], 16), m3)
        if kind == 'f0':
            return remote(k, 5, slot, shard.at[k, slot], region(k, blk, o['own'], 16), 1)
        name, rows, stage, mask = {'t2': ('pair', 32, 6, m2), 'f1': ('oth3', 16, 7, 1), 't1': ('quad', 64, 8, m1), 'f2': ('oth2', 32, 9, 1), 'f3': ('oth1', 64, 10, 1)}[kind]
        return remote(k, stage, slot, region(k, blk, o[name], rows), region(k, blk, o[name], rows), mask)

    starts = {4: ('loc', 't3', 'f0'), 5: ('t2', 'f1'), 6: ('t1', 'f2'), 7: ('f3',)}

    def wait_stage(k, stage, blk, slot, own):
        if stage == 0:
            load(k, blk, False)
            lslot = lax.rem(blk, 2)
            for half, dst in ((1 - core, snd0), (core, kp0)):
                lhs = lhs_v[k, lslot, :, pl.ds(pl.multiple_of(half * 128, 128), 128)]
                dst[k, own] = lax.dot_general(lhs, rhs_v[k, lslot], (((0,), (0,)), ((), ())), preferred_element_type=jnp.float32)
        elif stage <= 4:
            halves(k, stage - 1, slot, own).wait()
            if stage == 4:
                shard[k, slot] = (kp3[k, own] + rcv3[k, slot]) * (1.0 / N_DEV)
            else:
                rows = 128 >> stage
                side = bit(COLORS[k][stage - 1])
                keep, recv = kps[stage - 1], rcvs[stage - 1]
                for which, dst in ((1 - side, snds[stage]), (side, kps[stage])):
                    part = pl.ds(pl.multiple_of(which * rows, 16), rows)
                    dst[k, own] = keep[k, own, part, :] + recv[k, slot, part, :]
        else:
            for kind in starts[stage - 1]:
                gather(k, blk, slot, kind).wait()

    def start_stage(k, stage, blk, slot, own):
        if stage <= 3:
            halves(k, stage, slot, own).start()
        elif stage <= 7:
            for kind in starts[stage]:
                gather(k, blk, slot, kind).start()

    seq_len = qkv_v.shape[2]
    n_tok, width = dy_v.shape
    nt = (((1,), (1,)), ((), ()))

    def whole(which):
        src, dst = ((dy_b, dy_v), (hid_b, hid_v), (w_out.at[0], wo_v), (hid_v, dh_b))[which]
        return pltpu.make_async_copy(src, dst, whole_sem.at[which])

    def tile_loads(t, j):
        cols = pl.ds(pl.multiple_of((2 * t + j) * TILE, TILE), TILE)
        pairs = ((w_down.at[0, cols, :], w2_v.at[j]), (w_up.at[0, :, cols], w1_v.at[j]), (pre_b.at[:, cols], z_v.at[j]))
        return [pltpu.make_async_copy(src, dst, tile_sem.at[n, j]) for n, (src, dst) in enumerate(pairs)]

    def tile_store(t, j):
        cols = pl.ds(pl.multiple_of((2 * t + j) * TILE, TILE), TILE)
        return pltpu.make_async_copy(dz_v.at[j], dz_b.at[:, cols], tile_sem.at[3, j])

    def unit_place(t, i):
        unit = (t - N_TILE_STEP - 2) * UNITS + i
        per_seq = width // PAIR
        return unit < per_seq * (n_tok // seq_len), lax.div(unit, per_seq) * seq_len, lax.rem(unit, per_seq) * PAIR

    def unit_copies(t, i, load_it):
        _, row, col = unit_place(t, i)
        rows = pl.ds(pl.multiple_of(row, seq_len), seq_len)
        copies = []
        for part in range(3):
            cols = pl.ds(pl.multiple_of(part * width + col, PAIR), PAIR)
            if load_it:
                copies.append(pltpu.make_async_copy(qkv_b.at[rows, cols], qkv_v.at[i, part], head_sem.at[i, part]))
            else:
                copies.append(pltpu.make_async_copy(dqkv_v.at[i, part], dqkv_b.at[rows, cols], put_sem.at[i, part]))
        return copies

    def each_unit(t, body, units):
        for i in units:
            @pl.when(unit_place(t, i)[0])
            def _():
                body(i)

    def begin_tasks(t):
        @pl.when(t == 0)
        def _():
            whole(0).start()
            whole(1).start()

        @pl.when(t < N_TILE_STEP)
        def _():
            for j in range(2):
                for copy in tile_loads(t, j):
                    copy.start()

        @pl.when(t == N_TILE_STEP)
        def _():
            whole(2).start()

        @pl.when(t == N_TILE_STEP + 1)
        def _():
            whole(3).start()

        @pl.when((t >= N_TILE_STEP + 2) & (t < 16))
        def _():
            def loads(i):
                for copy in unit_copies(t, i, True):
                    copy.start()
            each_unit(t, loads, range(UNITS))

    def gelu_tile(t, j):
        for copy in tile_loads(t, j):
            copy.wait()
        d_act = lax.dot_general(dy_v[...], w2_v[j], nt, preferred_element_type=jnp.float32).astype(jnp.bfloat16).astype(jnp.float32)
        pre = z_v[j].astype(jnp.float32)
        inner = jnp.tanh(GELU_C * (pre + 0.044715 * (pre * pre * pre)))
        slope = 0.5 * (1.0 + inner) + 0.5 * pre * (1.0 - inner * inner) * (GELU_C * (1.0 + 3 * 0.044715 * (pre * pre)))
        dz_v[j] = (slope * d_act).astype(jnp.bfloat16)
        acc_v[...] += lax.dot_general(dz_v[j], w1_v[j], nt, preferred_element_type=jnp.float32)

    def norm_rows(n, _):
        rows = pl.ds(pl.multiple_of(n * 128, 128), 128)
        hid = hid_v[rows, :].astype(jnp.float32)
        d_norm = acc_v[rows, :].astype(jnp.bfloat16).astype(jnp.float32)
        inv = lax.rsqrt(jnp.mean(hid * hid, axis=-1, keepdims=True) + NORM_EPS)
        scaled = d_norm * gain_ref[...]
        d_hid = inv * scaled - hid * (inv * inv * inv * jnp.mean(scaled * hid, axis=-1, keepdims=True))
        dgain_ref[...] += jnp.sum((d_norm * (hid * inv)).reshape(16, 8, width), axis=0)
        hid_v[rows, :] = (dy_v[rows, :].astype(jnp.float32) + d_hid).astype(jnp.bfloat16)
        return 0

    def run_tasks(t):
        @pl.when(t == 0)
        def _():
            whole(0).wait()
            whole(1).wait()
            acc_v[...] = jnp.zeros_like(acc_v)
            dgain_ref[...] = jnp.zeros_like(dgain_ref)

        @pl.when(t < N_TILE_STEP)
        def _():
            for j in range(2):
                gelu_tile(t, j)
            for j in range(2):
                tile_store(t, j).start()
            for j in range(2):
                tile_store(t, j).wait()

        @pl.when(t == N_TILE_STEP)
        def _():
            lax.fori_loop(0, n_tok // 128, norm_rows, 0)

        @pl.when(t == N_TILE_STEP + 1)
        def _():
            whole(2).wait()
            for n in range(n_tok // 256):
                rows = pl.ds(n * 256, 256)
                dy_v[rows, :] = lax.dot_general(hid_v[rows, :], wo_v[...], nt, preferred_element_type=jnp.float32).astype(jnp.bfloat16)
            whole(3).wait()

        @pl.when((t >= N_TILE_STEP + 2) & (t < 16))
        def _():
            def compute(i):
                for copy in unit_copies(t, i, True):
                    copy.wait()
                _, row, col = unit_place(t, i)
                d_out = dy_v[pl.ds(pl.multiple_of(row, seq_len), seq_len), pl.ds(pl.multiple_of(col, PAIR), PAIR)]
                for part, vals in enumerate(pair_backward(qkv_v[i, 0], qkv_v[i, 1], qkv_v[i, 2], d_out)):
                    dqkv_v[i, part] = vals

            def begin_store(i):
                for copy in unit_copies(t, i, False):
                    copy.start()

            def end_store(i):
                for copy in unit_copies(t, i, False):
                    copy.wait()
            each_unit(t, compute, range(UNITS))
            for units in (range(UNITS - 1), range(UNITS - 1, UNITS)):
                each_unit(t, begin_store, units)
                each_unit(t, end_store, units)

    def step(t, _):
        begin_tasks(t)
        for phase in (wait_stage, start_stage):
            for stage in range(9):
                blk = t - 1 - stage * LAG

                @pl.when((blk >= 0) & (blk < N_BLOCK))
                def _():
                    for k in range(3):
                        phase(k, stage, blk, lax.rem(blk, SLOTS), lax.rem(blk, OWN_SLOTS))
            if phase is wait_stage:
                @pl.when(t < N_BLOCK)
                def _():
                    for k in range(3):
                        load(k, t, True)
        run_tasks(t)
        return 0

    lax.fori_loop(0, N_BLOCK + 1 + 8 * LAG, step, 0)


def reduce_gradients(operands, gain, n_layers, width, n_batch, seq_len):
    n_tok = n_batch * seq_len
    f32, bf16 = jnp.float32, jnp.bfloat16
    shapes = [((n_layers, 4 * width, width), f32), ((n_layers, width, 4 * width), f32), ((n_layers, width, 4 * width), f32),
              ((n_tok, 4 * width), bf16), ((n_tok, width), bf16), ((n_tok, 3 * width), bf16), ((8, width), f32)]
    scratch = [pltpu.VMEM((3, 2, n_tok, BLOCK), bf16), pltpu.VMEM((3, 2, n_tok, SQUARE), bf16)]
    for rows in (128, 64, 32, 16):
        scratch += [pltpu.VMEM((3, slots, rows, SQUARE), f32) for slots in (OWN_SLOTS, OWN_SLOTS, SLOTS)]
    scratch += [pltpu.VMEM((3, SLOTS, 16, SQUARE), f32)]
    scratch += [pltpu.VMEM((n_tok, width), bf16), pltpu.VMEM((n_tok, width), bf16), pltpu.VMEM((n_tok, width), f32),
                pltpu.VMEM((2, TILE, width), bf16), pltpu.VMEM((2, width, TILE), bf16), pltpu.VMEM((2, n_tok, TILE), bf16),
                pltpu.VMEM((2, n_tok, TILE), bf16), pltpu.VMEM((width, width), bf16), pltpu.VMEM((UNITS, 3, seq_len, PAIR), bf16),
                pltpu.VMEM((UNITS, 3, seq_len, PAIR), bf16)]
    scratch += [pltpu.SemaphoreType.DMA((3, 2, 2)), pltpu.SemaphoreType.DMA((3, SLOTS)),
                pltpu.SemaphoreType.DMA((3, 11, SLOTS)), pltpu.SemaphoreType.DMA((3, 11, SLOTS)),
                pltpu.SemaphoreType.DMA((4,)), pltpu.SemaphoreType.DMA((4, 2)), pltpu.SemaphoreType.DMA((UNITS, 3)), pltpu.SemaphoreType.DMA((UNITS, 3))]
    any_spec = pl.BlockSpec(memory_space=pl.ANY)
    vmem_spec = pl.BlockSpec(memory_space=pltpu.VMEM)
    return pl.pallas_call(
        reduce_kernel,
        out_shape=[jax.ShapeDtypeStruct(shape, dtype) for shape, dtype in shapes],
        in_specs=[any_spec] * len(operands) + [vmem_spec],
        out_specs=[any_spec] * 6 + [vmem_spec],
        scratch_shapes=scratch,
        cost_estimate=pl.CostEstimate(flops=600_000_000_000, bytes_accessed=400_000_000, transcendentals=0),
        compiler_params=pltpu.CompilerParams(collective_id=0, has_side_effects=True, vmem_limit_bytes=67_043_328),
        name="reduce_gradients",
    )(*operands, gain)


def add_small(vals):
    for mask in (1, 2, 4, 8):
        vals = vals + exchange(vals, mask)
    return vals * (1.0 / N_DEV)


def solution(mesh):
    def local_step(x_loc, grad_y_loc, gain_one, gain_two, w_qkv, w_out, w_up, w_down):
        n_layers, width = gain_one.shape
        n_batch, seq_len, _ = x_loc.shape
        x_blk = x_loc.reshape(n_batch * seq_len, width)
        saved_all = []
        for layer_idx in range(n_layers):
            norm_a, norm_a_back = jax.vjp(rms_gain, x_blk.astype(jnp.float32), gain_one[layer_idx])
            u_one = norm_a.astype(jnp.bfloat16)
            qkv_lo = dot_lo(u_one, w_qkv[layer_idx])
            attn_out = attention_forward(qkv_lo, n_batch, seq_len, width)
            hidden = x_blk + dot_lo(attn_out, w_out[layer_idx])
            norm_b, norm_b_back = jax.vjp(rms_gain, hidden.astype(jnp.float32), gain_two[layer_idx])
            u_two = norm_b.astype(jnp.bfloat16)
            pre_lo = dot_lo(u_two, w_up[layer_idx])
            act_f, gelu_back = jax.vjp(gelu_tanh, pre_lo.astype(jnp.float32))
            act_lo = act_f.astype(jnp.bfloat16)
            saved_all.append((norm_a_back, u_one, qkv_lo, attn_out, hidden, norm_b_back, u_two, pre_lo, gelu_back, act_lo))
            if layer_idx + 1 < n_layers:
                x_blk = hidden + dot_lo(act_lo, w_down[layer_idx])
        top_norm_back, top_u1, top_qkv, top_ao, _, top_norm_b_back, top_u2, _, top_gelu_back, top_act = saved_all[1]
        grad_top = grad_y_loc.reshape(n_batch * seq_len, width)
        (top_dz,) = top_gelu_back(dot_nt(grad_top, w_down[1]).astype(jnp.float32))
        top_dz = top_dz.astype(jnp.bfloat16)
        grad_h_norm, top_gain_b = top_norm_b_back(dot_nt(top_dz, w_up[1]).astype(jnp.float32))
        top_dh = (grad_top.astype(jnp.float32) + grad_h_norm).astype(jnp.bfloat16)
        top_dqkv = attention_backward(dot_nt(top_dh, w_out[1]), top_qkv, n_batch, seq_len, width)
        grad_x_norm, top_gain_a = top_norm_back(dot_nt(top_dqkv, w_qkv[1]).astype(jnp.float32))
        grad_mid = (top_dh.astype(jnp.float32) + grad_x_norm).astype(jnp.bfloat16)
        norm_a_back, u_one, qkv_lo, attn_out, hidden, _, u_two, pre_lo, _, act_lo = saved_all[0]
        operands = (top_act, act_lo, grad_top, grad_mid, top_u2, u_two, top_dz, top_u1, u_one, top_ao, attn_out, top_dqkv, top_dh,
                    pre_lo, hidden, qkv_lo, w_down, w_up, w_out)
        sum_down, sum_up, sum_attn, _, low_dh, low_dqkv, low_gain_b = reduce_gradients(operands, gain_two[:1], n_layers, width, n_batch, seq_len)
        grad_x_norm, low_gain_a = norm_a_back(dot_nt(low_dqkv, w_qkv[0]).astype(jnp.float32))
        grad_x = (low_dh.astype(jnp.float32) + grad_x_norm).astype(jnp.bfloat16)
        small = add_small(jnp.stack([low_gain_a, top_gain_a, jnp.sum(low_gain_b, axis=0), top_gain_b]))
        return grad_x.reshape(x_loc.shape), small[:n_layers], small[n_layers:], sum_attn[:, :, :3 * width], sum_attn[:, :, 3 * width:], sum_up, sum_down

    batch_spec = P('data')
    full_spec = P()
    return jax.shard_map(local_step, mesh=mesh, in_specs=(batch_spec, batch_spec) + (full_spec,) * 6, out_specs=(batch_spec,) + (full_spec,) * 6, check_vma=False)
```

```python
import functools

import jax
import jax.numpy as jnp
from jax import lax
from jax.experimental import pallas as pl
from jax.experimental.pallas import tpu as pltpu
from jax.sharding import PartitionSpec as P

NORM_EPS = 1e-6
GELU_C = 0.7978845608028654
HEAD_DIM = 64
N_DEV = 16

def rms_gain(rows_f, gain_vec):
    return rows_f * lax.rsqrt(jnp.mean(rows_f * rows_f, axis=-1, keepdims=True) + NORM_EPS) * gain_vec


def gelu_tanh(pre_act):
    return jax.nn.gelu(pre_act, approximate=True)


def dot_lo(lhs, rhs):
    return lax.dot_general(lhs, rhs, (((1,), (0,)), ((), ())), preferred_element_type=jnp.float32).astype(jnp.bfloat16)


def dot_nt(lhs, rhs):
    return lax.dot_general(lhs, rhs, (((1,), (1,)), ((), ())), preferred_element_type=jnp.float32).astype(jnp.bfloat16)


def dot_tn(lhs, rhs):
    return lax.dot_general(lhs, rhs, (((0,), (0,)), ((), ())), preferred_element_type=jnp.float32)


PAIR = 2 * HEAD_DIM
PAIRS_PER_STEP = 2


def head_mask(which, seq_len):
    lane = lax.broadcasted_iota(jnp.int32, (seq_len, PAIR), 1)
    return (lane >= which * HEAD_DIM) & (lane < (which + 1) * HEAD_DIM)


def one_head(rows, which):
    return jnp.where(head_mask(which, rows.shape[0]), rows, jnp.zeros_like(rows))


def head_probs(q_one, k_rows):
    seq_len = q_one.shape[0]
    scores = lax.dot_general(q_one, k_rows, (((1,), (1,)), ((), ())), preferred_element_type=jnp.float32) * HEAD_DIM ** -0.5
    row = lax.broadcasted_iota(jnp.int32, (seq_len, seq_len), 0)
    col = lax.broadcasted_iota(jnp.int32, (seq_len, seq_len), 1)
    scores = jnp.where(row >= col, scores, -1e30)
    expo = jnp.exp(scores - jnp.max(scores, axis=-1, keepdims=True))
    return expo * (1.0 / jnp.sum(expo, axis=-1, keepdims=True))


def pair_backward(q_rows, k_rows, v_rows, do_rows):
    tn = (((0,), (0,)), ((), ()))
    grads = []
    for which in range(2):
        q_one, do_one = one_head(q_rows, which), one_head(do_rows, which)
        prob = head_probs(q_one, k_rows)
        dprob = lax.dot_general(do_one, v_rows, (((1,), (1,)), ((), ())), preferred_element_type=jnp.float32)
        inner = jnp.sum(prob * dprob, axis=-1, keepdims=True)
        dscore = (prob * (dprob - inner) * HEAD_DIM ** -0.5).astype(jnp.bfloat16)
        dq = jnp.dot(dscore, k_rows, preferred_element_type=jnp.float32)
        dk = lax.dot_general(dscore, q_one, tn, preferred_element_type=jnp.float32)
        dv = lax.dot_general(prob.astype(jnp.bfloat16), do_one, tn, preferred_element_type=jnp.float32)
        grads.append((dq, dk, dv))
    mask = head_mask(0, q_rows.shape[0])
    return [jnp.where(mask, one, two).astype(jnp.bfloat16) for one, two in zip(*grads)]


def attn_fwd_kernel(q_ref, k_ref, v_ref, o_ref):
    mask = head_mask(0, q_ref.shape[0])
    for pair in range(PAIRS_PER_STEP):
        cols = pl.ds(pair * PAIR, PAIR)
        both = []
        for which in range(2):
            prob = head_probs(one_head(q_ref[:, cols], which), k_ref[:, cols]).astype(jnp.bfloat16)
            both.append(jnp.dot(prob, v_ref[:, cols], preferred_element_type=jnp.float32))
        o_ref[:, cols] = jnp.where(mask, both[0], both[1]).astype(jnp.bfloat16)


def attn_bwd_kernel(q_ref, k_ref, v_ref, do_ref, dqkv_ref):
    seq_len = q_ref.shape[0]
    width = dqkv_ref.shape[1] // 3
    row0 = pl.multiple_of(pl.program_id(0) * seq_len, seq_len)
    for pair in range(PAIRS_PER_STEP):
        cols = pl.ds(pair * PAIR, PAIR)
        col0 = pl.multiple_of((pl.program_id(1) * PAIRS_PER_STEP + pair) * PAIR, PAIR)
        grads = pair_backward(q_ref[:, cols], k_ref[:, cols], v_ref[:, cols], do_ref[:, cols])
        for part, vals in enumerate(grads):
            dqkv_ref[pl.ds(row0, seq_len), pl.ds(part * width + col0, PAIR)] = vals


def head_specs(seq_len, n_step, lanes):
    return [pl.BlockSpec((seq_len, lanes), functools.partial(lambda part, b, h: (b, part * n_step + h), part)) for part in range(3)]


def attention_forward(qkv_lo, n_batch, seq_len, width):
    lanes = PAIR * PAIRS_PER_STEP
    n_step = width // lanes
    n_tok = n_batch * seq_len
    return pl.pallas_call(
        attn_fwd_kernel,
        grid=(n_batch, n_step),
        in_specs=head_specs(seq_len, n_step, lanes),
        out_specs=pl.BlockSpec((seq_len, lanes), lambda b, h: (b, h)),
        out_shape=jax.ShapeDtypeStruct((n_tok, width), jnp.bfloat16),
        cost_estimate=pl.CostEstimate(flops=14_000_000_000, bytes_accessed=6_300_000, transcendentals=4_700_000),
        compiler_params=pltpu.CompilerParams(dimension_semantics=("arbitrary", "arbitrary")),
        name="attn_fwd",
    )(qkv_lo, qkv_lo, qkv_lo)


def attention_backward(grad_attn, qkv_lo, n_batch, seq_len, width):
    lanes = PAIR * PAIRS_PER_STEP
    n_step = width // lanes
    n_tok = n_batch * seq_len
    return pl.pallas_call(
        attn_bwd_kernel,
        grid=(n_batch, n_step),
        in_specs=head_specs(seq_len, n_step, lanes) + [pl.BlockSpec((seq_len, lanes), lambda b, h: (b, h))],
        out_specs=pl.BlockSpec((n_tok, 3 * width), lambda b, h: (0, 0)),
        out_shape=jax.ShapeDtypeStruct((n_tok, 3 * width), jnp.bfloat16),
        cost_estimate=pl.CostEstimate(flops=40_000_000_000, bytes_accessed=12_600_000, transcendentals=4_700_000),
        compiler_params=pltpu.CompilerParams(dimension_semantics=("arbitrary", "arbitrary")),
        name="attn_bwd",
    )(qkv_lo, qkv_lo, qkv_lo, grad_attn)


N_BLOCK = 32
LAG = 2
SLOTS = 2 * LAG
OWN_SLOTS = LAG + 1
TILE = 256
UNITS = 3
T_MLP = 3
T_NORM = T_MLP + 8
T_HEAD = T_NORM + 2
T_IN = T_HEAD + 8
T_LAST = T_IN + 6
T_SMALL = T_LAST + 2
BLOCK = 256
SQUARE = 1024
COLORS = ((2, 4, 8), (4, 8, 2), (8, 2, 4))
MESH_ID = pl.DeviceIdType.MESH


def reduce_kernel(*refs):
    (act_t, act_b, dy_t, dy_b, u2_t, u2_b, dz_t, u1_t, u1_b, ao_t, ao_b, dqkv_t, dh_t, pre_b, hid_b, qkv_b, x_b, w_down, w_up, w_out, w_qkv, gain_ref, top_gain_ref,
     out_a, out_b, out_c, dz_b, dh_b, dqkv_b, dx_b, small_ref, lhs_v, rhs_v, snd0, kp0, rcv0, snd1, kp1, rcv1, snd2, kp2, rcv2, snd3, kp3, rcv3, shard,
     dy_v, hid_v, acc_v, w2_v, w1_v, z_v, dz_v, wo_v, qkv_v, dqkv_v, dgain_v, part_v, peer_v,
     load_sem, loc_sem, send_sem, recv_sem, whole_sem, tile_sem, head_sem, put_sem, small_send, small_recv) = refs
    me = lax.axis_index('data')
    outs = (out_a, out_b, out_c)
    snds, kps, rcvs = (snd0, snd1, snd2, snd3), (kp0, kp1, kp2, kp3), (rcv0, rcv1, rcv2, rcv3)

    def bit(mask):
        return lax.rem(lax.div(me, mask), 2)

    def peer(mask):
        return me + mask * (1 - 2 * bit(mask))

    core = bit(1)
    barrier = pltpu.get_barrier_semaphore()
    for mask in (1, 2, 4, 8):
        pl.semaphore_signal(barrier, inc=1, device_id=(peer(mask),), device_id_type=MESH_ID)
    pl.semaphore_wait(barrier, 4)

    def place(k, blk):
        top = lax.div(blk, 16)
        sq = lax.div(lax.rem(blk, 16), 4)
        if k == 2:
            sq = lax.rem(sq + 3 * top, 4)
        return top, sq, lax.rem(blk, 4)

    def region(k, blk, off, rows):
        top, sq, quarter = place(k, blk)
        layer = 1 - top
        row = quarter * BLOCK + off
        if k == 0:
            return outs[k].at[layer, pl.ds(pl.multiple_of(sq * SQUARE + row, 16), rows), :]
        return outs[k].at[layer, pl.ds(pl.multiple_of(row, 16), rows), pl.ds(pl.multiple_of(sq * SQUARE, SQUARE), SQUARE)]

    def load(k, blk, start):
        top, sq, quarter = place(k, blk)
        slot = lax.rem(blk, 2)
        dst_l, dst_r = lhs_v.at[k, slot], rhs_v.at[k, slot]

        def copies(lhs, rhs, lhs_col, rhs_col):
            return (pltpu.make_async_copy(lhs.at[:, pl.ds(pl.multiple_of(lhs_col, BLOCK), BLOCK)], dst_l, load_sem.at[k, slot, 0]),
                    pltpu.make_async_copy(rhs.at[:, pl.ds(pl.multiple_of(rhs_col, SQUARE), SQUARE)], dst_r, load_sem.at[k, slot, 1]))

        if not start:
            for copy in copies(u2_t, dz_t, 0, 0):
                copy.wait()
            return
        if k == 0:
            pairs = [(top == 0, act_t, dy_t, sq * SQUARE + quarter * BLOCK, 0), (top == 1, act_b, dy_b, sq * SQUARE + quarter * BLOCK, 0)]
        elif k == 1:
            pairs = [(top == 0, u2_t, dz_t, quarter * BLOCK, sq * SQUARE), (top == 1, u2_b, dz_b, quarter * BLOCK, sq * SQUARE)]
        else:
            pairs = [((top == 0) & (sq < 3), u1_t, dqkv_t, quarter * BLOCK, sq * SQUARE), ((top == 0) & (sq == 3), ao_t, dh_t, quarter * BLOCK, 0),
                     ((top == 1) & (sq < 3), u1_b, dqkv_b, quarter * BLOCK, sq * SQUARE), ((top == 1) & (sq == 3), ao_b, dh_b, quarter * BLOCK, 0)]
        for cond, lhs, rhs, lhs_col, rhs_col in pairs:
            @pl.when(cond)
            def _():
                for copy in copies(lhs, rhs, lhs_col, rhs_col):
                    copy.start()

    def remote(k, stage, slot, src, dst, mask):
        return pltpu.make_async_remote_copy(src_ref=src, dst_ref=dst, send_sem=send_sem.at[k, stage, slot], recv_sem=recv_sem.at[k, stage, slot],
                                            device_id=(peer(mask),), device_id_type=MESH_ID)

    def halves(k, stage, slot, own):
        mask = (1,) + COLORS[k]
        return remote(k, stage, slot, snds[stage].at[k, own], rcvs[stage].at[k, slot], mask[stage])

    def offs(k):
        m1, m2, m3 = COLORS[k]
        b1, b2, b3 = bit(m1), bit(m2), bit(m3)
        base = core * 128
        return dict(own=base + b1 * 64 + b2 * 32 + b3 * 16, oth3=base + b1 * 64 + b2 * 32 + (1 - b3) * 16, pair=base + b1 * 64 + b2 * 32,
                    oth2=base + b1 * 64 + (1 - b2) * 32, quad=base + b1 * 64, oth1=base + (1 - b1) * 64)

    def gather(k, blk, slot, kind):
        o, (m1, m2, m3) = offs(k), COLORS[k]
        if kind == 'loc':
            return pltpu.make_async_copy(shard.at[k, slot], region(k, blk, o['own'], 16), loc_sem.at[k, slot])
        if kind == 't3':
            return remote(k, 4, slot, shard.at[k, slot], region(k, blk, o['own'], 16), m3)
        if kind == 'f0':
            return remote(k, 5, slot, shard.at[k, slot], region(k, blk, o['own'], 16), 1)
        name, rows, stage, mask = {'t2': ('pair', 32, 6, m2), 'f1': ('oth3', 16, 7, 1), 't1': ('quad', 64, 8, m1), 'f2': ('oth2', 32, 9, 1), 'f3': ('oth1', 64, 10, 1)}[kind]
        return remote(k, stage, slot, region(k, blk, o[name], rows), region(k, blk, o[name], rows), mask)

    starts = {4: ('loc', 't3', 'f0'), 5: ('t2', 'f1'), 6: ('t1', 'f2'), 7: ('f3',)}

    def wait_stage(k, stage, blk, slot, own):
        if stage == 0:
            load(k, blk, False)
            lslot = lax.rem(blk, 2)
            for half, dst in ((1 - core, snd0), (core, kp0)):
                lhs = lhs_v[k, lslot, :, pl.ds(pl.multiple_of(half * 128, 128), 128)]
                dst[k, own] = lax.dot_general(lhs, rhs_v[k, lslot], (((0,), (0,)), ((), ())), preferred_element_type=jnp.float32)
        elif stage <= 4:
            halves(k, stage - 1, slot, own).wait()
            if stage == 4:
                shard[k, slot] = (kp3[k, own] + rcv3[k, slot]) * (1.0 / N_DEV)
            else:
                rows = 128 >> stage
                side = bit(COLORS[k][stage - 1])
                keep, recv = kps[stage - 1], rcvs[stage - 1]
                for which, dst in ((1 - side, snds[stage]), (side, kps[stage])):
                    part = pl.ds(pl.multiple_of(which * rows, 16), rows)
                    dst[k, own] = keep[k, own, part, :] + recv[k, slot, part, :]
        else:
            for kind in starts[stage - 1]:
                gather(k, blk, slot, kind).wait()

    def start_stage(k, stage, blk, slot, own):
        if stage <= 3:
            halves(k, stage, slot, own).start()
        elif stage <= 7:
            for kind in starts[stage]:
                gather(k, blk, slot, kind).start()

    seq_len = qkv_v.shape[2]
    n_tok, width = dy_v.shape
    nt = (((1,), (1,)), ((), ()))

    def whole(which):
        src, dst = ((dy_b, dy_v), (hid_b, hid_v), (w_out.at[0], wo_v), (hid_v, dh_b), (x_b, dy_v), (hid_v, dx_b))[which]
        return pltpu.make_async_copy(src, dst, whole_sem.at[which])

    def tile_loads(t, j):
        cols = pl.ds(pl.multiple_of((2 * (t - T_MLP) + j) * TILE, TILE), TILE)
        pairs = ((w_down.at[0, cols, :], w2_v.at[j]), (w_up.at[0, :, cols], w1_v.at[j]), (pre_b.at[:, cols], z_v.at[j]))
        return [pltpu.make_async_copy(src, dst, tile_sem.at[n, j]) for n, (src, dst) in enumerate(pairs)]

    def in_loads(t, j):
        cols = pl.ds(pl.multiple_of((2 * (t - T_IN) + j) * TILE, TILE), TILE)
        pairs = ((w_qkv.at[0, :, cols], w1_v.at[j]), (dqkv_b.at[:, cols], z_v.at[j]))
        return [pltpu.make_async_copy(src, dst, tile_sem.at[n + 1, j]) for n, (src, dst) in enumerate(pairs)]

    def small_copy(n):
        return pltpu.make_async_remote_copy(src_ref=part_v.at[n], dst_ref=peer_v.at[n], send_sem=small_send.at[n], recv_sem=small_recv.at[n],
                                            device_id=(peer(1 << n),), device_id_type=MESH_ID)

    def tile_store(t, j):
        cols = pl.ds(pl.multiple_of((2 * (t - T_MLP) + j) * TILE, TILE), TILE)
        return pltpu.make_async_copy(dz_v.at[j], dz_b.at[:, cols], tile_sem.at[3, j])

    def unit_place(t, i):
        unit = (t - T_HEAD) * UNITS + i
        per_seq = width // PAIR
        return unit < per_seq * (n_tok // seq_len), lax.div(unit, per_seq) * seq_len, lax.rem(unit, per_seq) * PAIR

    def unit_copies(t, i, load_it):
        _, row, col = unit_place(t, i)
        rows = pl.ds(pl.multiple_of(row, seq_len), seq_len)
        copies = []
        for part in range(3):
            cols = pl.ds(pl.multiple_of(part * width + col, PAIR), PAIR)
            if load_it:
                copies.append(pltpu.make_async_copy(qkv_b.at[rows, cols], qkv_v.at[i, part], head_sem.at[i, part]))
            else:
                copies.append(pltpu.make_async_copy(dqkv_v.at[i, part], dqkv_b.at[rows, cols], put_sem.at[i, part]))
        return copies

    def each_unit(t, body, units):
        for i in units:
            @pl.when(unit_place(t, i)[0])
            def _():
                body(i)

    def begin_tasks(t):
        for when, which in ((T_MLP, 0), (T_MLP, 1), (T_NORM, 2), (T_IN, 4)):
            @pl.when(t == when)
            def _():
                whole(which).start()

        for first, last, copies in ((T_MLP, T_NORM, tile_loads), (T_IN, T_LAST, in_loads)):
            @pl.when((t >= first) & (t < last))
            def _():
                for j in range(2):
                    for copy in copies(t, j):
                        copy.start()

        @pl.when((t >= T_HEAD) & (t < T_IN - 1))
        def _():
            def loads(i):
                for copy in unit_copies(t, i, True):
                    copy.start()
            each_unit(t, loads, range(UNITS))

    def gelu_tile(t, j):
        for copy in tile_loads(t, j):
            copy.wait()
        d_act = lax.dot_general(dy_v[...], w2_v[j], nt, preferred_element_type=jnp.float32).astype(jnp.bfloat16).astype(jnp.float32)
        pre = z_v[j].astype(jnp.float32)
        inner = jnp.tanh(GELU_C * (pre + 0.044715 * (pre * pre * pre)))
        slope = 0.5 * (1.0 + inner) + 0.5 * pre * (1.0 - inner * inner) * (GELU_C * (1.0 + 3 * 0.044715 * (pre * pre)))
        dz_v[j] = (slope * d_act).astype(jnp.bfloat16)
        acc_v[...] += lax.dot_general(dz_v[j], w1_v[j], nt, preferred_element_type=jnp.float32)

    def norm_backward(src, residual, which):
        def norm_rows(n, _):
            rows = pl.ds(pl.multiple_of(n * 128, 128), 128)
            hid = src[rows, :].astype(jnp.float32)
            d_norm = acc_v[rows, :].astype(jnp.bfloat16).astype(jnp.float32)
            inv = lax.rsqrt(jnp.mean(hid * hid, axis=-1, keepdims=True) + NORM_EPS)
            scaled = d_norm * gain_ref[which:which + 1, :]
            d_hid = inv * scaled - hid * (inv * inv * inv * jnp.mean(scaled * hid, axis=-1, keepdims=True))
            dgain_v[which] += jnp.sum((d_norm * (hid * inv)).reshape(16, 8, width), axis=0)
            hid_v[rows, :] = (residual[rows, :].astype(jnp.float32) + d_hid).astype(jnp.bfloat16)
            return 0
        lax.fori_loop(0, n_tok // 128, norm_rows, 0)

    def run_tasks(t):
        @pl.when(t == T_MLP)
        def _():
            whole(0).wait()
            whole(1).wait()
            dgain_v[...] = jnp.zeros_like(dgain_v)

        @pl.when((t == T_MLP) | (t == T_IN))
        def _():
            acc_v[...] = jnp.zeros_like(acc_v)

        @pl.when((t >= T_MLP) & (t < T_NORM))
        def _():
            for j in range(2):
                gelu_tile(t, j)
            for j in range(2):
                tile_store(t, j).start()
            for j in range(2):
                tile_store(t, j).wait()

        @pl.when(t == T_NORM)
        def _():
            norm_backward(hid_v, dy_v, 0)

        @pl.when(t == T_NORM + 1)
        def _():
            whole(3).start()
            whole(2).wait()
            for n in range(n_tok // 256):
                rows = pl.ds(n * 256, 256)
                dy_v[rows, :] = lax.dot_general(hid_v[rows, :], wo_v[...], nt, preferred_element_type=jnp.float32).astype(jnp.bfloat16)
            whole(3).wait()

        @pl.when(t == T_IN)
        def _():
            whole(4).wait()

        @pl.when((t >= T_IN) & (t < T_LAST))
        def _():
            for j in range(2):
                for copy in in_loads(t, j):
                    copy.wait()
                acc_v[...] += lax.dot_general(z_v[j], w1_v[j], nt, preferred_element_type=jnp.float32)

        @pl.when(t == T_LAST)
        def _():
            norm_backward(dy_v, hid_v, 1)

        @pl.when(t == T_LAST + 1)
        def _():
            whole(5).start()
            row = lax.broadcasted_iota(jnp.int32, (8, width), 0)
            low = [jnp.sum(dgain_v[n], axis=0, keepdims=True) for n in range(2)]
            part_v[0] = jnp.where(row == 0, low[1], jnp.where(row == 2, low[0], top_gain_ref[...]))
            whole(5).wait()

        for n in range(4):
            @pl.when(t == T_SMALL + 2 * n)
            def _():
                small_copy(n).start()

            @pl.when(t == T_SMALL + 2 * n + 1)
            def _():
                small_copy(n).wait()
                total = part_v[n] + peer_v[n]
                if n < 3:
                    part_v[n + 1] = total
                else:
                    small_ref[...] = total * (1.0 / N_DEV)

        @pl.when((t >= T_HEAD) & (t < T_IN - 1))
        def _():
            def compute(i):
                for copy in unit_copies(t, i, True):
                    copy.wait()
                _, row, col = unit_place(t, i)
                d_out = dy_v[pl.ds(pl.multiple_of(row, seq_len), seq_len), pl.ds(pl.multiple_of(col, PAIR), PAIR)]
                for part, vals in enumerate(pair_backward(qkv_v[i, 0], qkv_v[i, 1], qkv_v[i, 2], d_out)):
                    dqkv_v[i, part] = vals

            def begin_store(i):
                for copy in unit_copies(t, i, False):
                    copy.start()

            def end_store(i):
                for copy in unit_copies(t, i, False):
                    copy.wait()
            each_unit(t, compute, range(UNITS))
            for units in (range(UNITS - 1), range(UNITS - 1, UNITS)):
                each_unit(t, begin_store, units)
                each_unit(t, end_store, units)

    def step(t, _):
        begin_tasks(t)
        for phase in (wait_stage, start_stage):
            for stage in range(9):
                blk = t - 1 - stage * LAG

                @pl.when((blk >= 0) & (blk < N_BLOCK))
                def _():
                    for k in range(3):
                        phase(k, stage, blk, lax.rem(blk, SLOTS), lax.rem(blk, OWN_SLOTS))
            if phase is wait_stage:
                @pl.when(t < N_BLOCK)
                def _():
                    for k in range(3):
                        load(k, t, True)
        run_tasks(t)
        return 0

    lax.fori_loop(0, N_BLOCK + 1 + 8 * LAG, step, 0)


def reduce_gradients(operands, gains, top_gains, n_layers, width, n_batch, seq_len):
    n_tok = n_batch * seq_len
    f32, bf16 = jnp.float32, jnp.bfloat16
    shapes = [((n_layers, 4 * width, width), f32), ((n_layers, width, 4 * width), f32), ((n_layers, width, 4 * width), f32),
              ((n_tok, 4 * width), bf16), ((n_tok, width), bf16), ((n_tok, 3 * width), bf16), ((n_tok, width), bf16), ((8, width), f32)]
    scratch = [pltpu.VMEM((3, 2, n_tok, BLOCK), bf16), pltpu.VMEM((3, 2, n_tok, SQUARE), bf16)]
    for rows in (128, 64, 32, 16):
        scratch += [pltpu.VMEM((3, slots, rows, SQUARE), f32) for slots in (OWN_SLOTS, OWN_SLOTS, SLOTS)]
    scratch += [pltpu.VMEM((3, SLOTS, 16, SQUARE), f32)]
    scratch += [pltpu.VMEM((n_tok, width), bf16), pltpu.VMEM((n_tok, width), bf16), pltpu.VMEM((n_tok, width), f32),
                pltpu.VMEM((2, TILE, width), bf16), pltpu.VMEM((2, width, TILE), bf16), pltpu.VMEM((2, n_tok, TILE), bf16),
                pltpu.VMEM((2, n_tok, TILE), bf16), pltpu.VMEM((width, width), bf16), pltpu.VMEM((UNITS, 3, seq_len, PAIR), bf16),
                pltpu.VMEM((UNITS, 3, seq_len, PAIR), bf16), pltpu.VMEM((2, 8, width), f32), pltpu.VMEM((4, 8, width), f32), pltpu.VMEM((4, 8, width), f32)]
    scratch += [pltpu.SemaphoreType.DMA((3, 2, 2)), pltpu.SemaphoreType.DMA((3, SLOTS)),
                pltpu.SemaphoreType.DMA((3, 11, SLOTS)), pltpu.SemaphoreType.DMA((3, 11, SLOTS)),
                pltpu.SemaphoreType.DMA((6,)), pltpu.SemaphoreType.DMA((4, 2)), pltpu.SemaphoreType.DMA((UNITS, 3)), pltpu.SemaphoreType.DMA((UNITS, 3)),
                pltpu.SemaphoreType.DMA((4,)), pltpu.SemaphoreType.DMA((4,))]
    any_spec = pl.BlockSpec(memory_space=pl.ANY)
    vmem_spec = pl.BlockSpec(memory_space=pltpu.VMEM)
    return pl.pallas_call(
        reduce_kernel,
        out_shape=[jax.ShapeDtypeStruct(shape, dtype) for shape, dtype in shapes],
        in_specs=[any_spec] * len(operands) + [vmem_spec] * 2,
        out_specs=[any_spec] * 7 + [vmem_spec],
        scratch_shapes=scratch,
        cost_estimate=pl.CostEstimate(flops=600_000_000_000, bytes_accessed=400_000_000, transcendentals=0),
        compiler_params=pltpu.CompilerParams(collective_id=0, has_side_effects=True, vmem_limit_bytes=67_043_328),
        name="reduce_gradients",
    )(*operands, gains, top_gains)


def solution(mesh):
    def local_step(x_loc, grad_y_loc, gain_one, gain_two, w_qkv, w_out, w_up, w_down):
        n_layers, width = gain_one.shape
        n_batch, seq_len, _ = x_loc.shape
        x_blk = x_loc.reshape(n_batch * seq_len, width)
        saved_all = []
        for layer_idx in range(n_layers):
            norm_a, norm_a_back = jax.vjp(rms_gain, x_blk.astype(jnp.float32), gain_one[layer_idx])
            u_one = norm_a.astype(jnp.bfloat16)
            qkv_lo = dot_lo(u_one, w_qkv[layer_idx])
            attn_out = attention_forward(qkv_lo, n_batch, seq_len, width)
            hidden = x_blk + dot_lo(attn_out, w_out[layer_idx])
            norm_b, norm_b_back = jax.vjp(rms_gain, hidden.astype(jnp.float32), gain_two[layer_idx])
            u_two = norm_b.astype(jnp.bfloat16)
            pre_lo = dot_lo(u_two, w_up[layer_idx])
            act_f, gelu_back = jax.vjp(gelu_tanh, pre_lo.astype(jnp.float32))
            act_lo = act_f.astype(jnp.bfloat16)
            saved_all.append((norm_a_back, u_one, qkv_lo, attn_out, hidden, norm_b_back, u_two, pre_lo, gelu_back, act_lo))
            if layer_idx + 1 < n_layers:
                x_blk = hidden + dot_lo(act_lo, w_down[layer_idx])
        top_norm_back, top_u1, top_qkv, top_ao, _, top_norm_b_back, top_u2, _, top_gelu_back, top_act = saved_all[1]
        grad_top = grad_y_loc.reshape(n_batch * seq_len, width)
        (top_dz,) = top_gelu_back(dot_nt(grad_top, w_down[1]).astype(jnp.float32))
        top_dz = top_dz.astype(jnp.bfloat16)
        grad_h_norm, top_gain_b = top_norm_b_back(dot_nt(top_dz, w_up[1]).astype(jnp.float32))
        top_dh = (grad_top.astype(jnp.float32) + grad_h_norm).astype(jnp.bfloat16)
        top_dqkv = attention_backward(dot_nt(top_dh, w_out[1]), top_qkv, n_batch, seq_len, width)
        grad_x_norm, top_gain_a = top_norm_back(dot_nt(top_dqkv, w_qkv[1]).astype(jnp.float32))
        grad_mid = (top_dh.astype(jnp.float32) + grad_x_norm).astype(jnp.bfloat16)
        _, u_one, qkv_lo, attn_out, hidden, _, u_two, pre_lo, _, act_lo = saved_all[0]
        operands = (top_act, act_lo, grad_top, grad_mid, top_u2, u_two, top_dz, top_u1, u_one, top_ao, attn_out, top_dqkv, top_dh,
                    pre_lo, hidden, qkv_lo, x_loc.reshape(n_batch * seq_len, width), w_down, w_up, w_out, w_qkv)
        zero = jnp.zeros_like(top_gain_a)
        top_gains = jnp.stack([zero, top_gain_a, zero, top_gain_b] + [zero] * 4)
        gains = jnp.concatenate([gain_two[:1], gain_one[:1]])
        sums = reduce_gradients(operands, gains, top_gains, n_layers, width, n_batch, seq_len)
        sum_down, sum_up, sum_attn, grad_x, small = sums[0], sums[1], sums[2], sums[6], sums[7]
        return grad_x.reshape(x_loc.shape), small[:2], small[2:4], sum_attn[:, :, :3 * width], sum_attn[:, :, 3 * width:], sum_up, sum_down

    batch_spec = P('data')
    full_spec = P()
    return jax.shard_map(local_step, mesh=mesh, in_specs=(batch_spec, batch_spec) + (full_spec,) * 6, out_specs=(batch_spec,) + (full_spec,) * 6, check_vma=False)
```
